8 devices in a mesh: dp: 2 (over y, z), tp: 4 (over x, core).
Axes of the slice: x: 2, y: 2, z: 1, core: 2. Of those that a mesh axis runs over, the one named last changes fastest.
Arguments:
- x: bfloat16 [4096, 2048], P(('dp', 'tp')), parts along dimension 0
- gain: bfloat16 [2048], replicated
- wq: bfloat16 [2048, 3072], P(None, 'tp')
- wk: bfloat16 [2048, 3072], P(None, 'tp')
- wv: bfloat16 [2048, 3072], P(None, 'tp')
- wo: bfloat16 [3072, 2048], P('tp')
Outputs:
- output: bfloat16 [4096, 2048], P(('dp', 'tp')), parts along dimension 0
There are 2 independent parts. The reference program is written for one: setup_inputs(seed, part) draws one part's arguments, and reference() takes and returns one part's arrays. A program takes and returns all parts, laid end to end along the dimension named above; an argument that names none is the same for every part.
All inputs are finite; a program needn't handle non-finite values.
Results may differ from the reference program's by a relative error of at most 0.012.
Values are sent between devices in bfloat16 or wider.
A program may use at most 2 GiB of HBM per device.

```python
import jax
import jax.numpy as jnp
from jax import lax

ROWS = 2048
D = 2048
HEADS = 24
KV_HEADS = 24
HEAD = 128
THETA = 10000


def setup_inputs(seed: int = 0, part: int = 0) -> dict:
    kx, kn, kq, kk, kv, ko = jax.random.split(jax.random.key(seed), 6)

    def weights(key, rows, columns):
        return jax.random.normal(key, (rows, columns), jnp.float32) * rows**-0.5

    drawn = {
        "x": jax.random.normal(jax.random.fold_in(kx, part), (ROWS, D), jnp.float32),
        "gain": 1 + 0.1 * jax.random.normal(kn, (D,), jnp.float32),
        "wq": 2 * weights(kq, D, HEADS * HEAD),
        "wk": 2 * weights(kk, D, KV_HEADS * HEAD),
        "wv": 4 * weights(kv, D, KV_HEADS * HEAD),
        "wo": weights(ko, HEADS * HEAD, D),
    }
    return {k: v.astype(jnp.bfloat16) for k, v in drawn.items()}


def normed(x, gain):
    wide = x.astype(jnp.float32)
    scale = lax.rsqrt(jnp.mean(wide * wide, -1, keepdims=True) + 1e-6)
    return (wide * scale * gain.astype(jnp.float32)).astype(jnp.bfloat16)


def turned(t, place, theta):
    half = t.shape[-1] // 2
    angle = place.astype(jnp.float32)[:, None] * theta ** (-jnp.arange(half, dtype=jnp.float32) / half)
    cos, sin = jnp.cos(angle)[:, None], jnp.sin(angle)[:, None]
    a, b = t[..., :half].astype(jnp.float32), t[..., half:].astype(jnp.float32)
    return jnp.concatenate([a * cos - b * sin, b * cos + a * sin], -1).astype(jnp.bfloat16)


def matmul(a, w):
    return jnp.dot(a, w, preferred_element_type=jnp.float32).astype(jnp.bfloat16)


def einsum(form, a, b):
    return jnp.einsum(form, a.astype(jnp.float32), b.astype(jnp.float32))


def attention(q, k, v):
    scores = einsum("tgsd,ugd->gstu", q, k) * q.shape[-1] ** -0.5
    token = jnp.arange(q.shape[0])
    scores = jnp.where(token[:, None] >= token, scores, -jnp.inf)
    weights = jax.nn.softmax(scores, -1).astype(jnp.bfloat16)
    return einsum("gstu,ugd->tgsd", weights, v).astype(jnp.bfloat16)


def reference(x, gain, wq, wk, wv, wo):
    a, place = normed(x, gain), jnp.arange(ROWS)
    q = turned(matmul(a, wq).reshape(ROWS, HEADS, HEAD), place, THETA).reshape(ROWS, KV_HEADS, -1, HEAD)
    k = turned(matmul(a, wk).reshape(ROWS, KV_HEADS, HEAD), place, THETA)
    v = matmul(a, wv).reshape(ROWS, KV_HEADS, HEAD)
    seen = attention(q, k, v).reshape(ROWS, HEADS * HEAD)
    return (x.astype(jnp.float32) + jnp.dot(seen, wo, preferred_element_type=jnp.float32)).astype(jnp.bfloat16)
```

```python
import functools

import jax
import jax.numpy as jnp
import numpy as np
from jax import lax
from jax.experimental import pallas as pl
from jax.experimental.pallas import tpu as pltpu
from jax.sharding import PartitionSpec as P

HEAD = 128
THETA = 10000
NEG = -1e30
HIDDEN = 2 * NEG
LOG2E = 1.4426950408889634
MESH = pl.DeviceIdType.MESH
BLOCK = 256
HALF = BLOCK // 2
PAD = 16


def _dot(a, b, ca, cb):
    return lax.dot_general(a, b, (((ca,), (cb,)), ((), ())), preferred_element_type=jnp.float32)


def _aligned(x, n):
    return pl.multiple_of(x, n)


def kernel(own, x_hbm, gain_ref, wq_hbm, wk_hbm, wv_hbm, wo_hbm, cos_in, sin_in, cos_at, sin_at, y_hbm,
           x_s, xn_s, w_s, wo_s, q_s, k_s, vt_s, seen_s, top_s, mix_s, term_s, got_s, acc_s, y_s,
           load_sem, out_sem, near_send, near_recv, far_send, far_recv, pass_send, pass_recv,
           seen_send, seen_recv, mine_send, mine_recv, wo_send, wo_recv, term_send, term_recv):
    heads = q_s.shape[0]
    width = x_s.shape[1]
    inner = heads * HEAD
    tp = lax.axis_index("tp")
    c = lax.rem(tp, 2)
    chip = lax.div(tp, 2)
    mate = tp + 1 - 2 * c
    peer = lax.rem(tp + 2, 4)
    here = chip * (2 * own)
    there = (1 - chip) * (2 * own)
    mine = here + c * own
    mates = here + (1 - c) * own

    def remote(src, dst, send, recv, device):
        return pltpu.make_async_remote_copy(src_ref=src, dst_ref=dst, send_sem=send, recv_sem=recv, device_id={"tp": device}, device_id_type=MESH)

    def load_x(i):
        rows = pl.ds(i * HALF, HALF)
        return pltpu.make_async_copy(x_hbm.at[rows, :], x_s.at[rows, :], load_sem.at[i])

    def load_w(i):
        return pltpu.make_async_copy((wq_hbm, wk_hbm, wv_hbm)[i], w_s.at[i], load_sem.at[4 + i])

    load_wo = pltpu.make_async_copy(wo_hbm, wo_s.at[c], load_sem.at[7])
    for i in range(4):
        load_x(i).start()
    for i in range(3):
        load_w(i).start()
    load_wo.start()

    barrier = pltpu.get_barrier_semaphore()
    for other in range(1, 4):
        pl.semaphore_signal(barrier, inc=1, device_id={"tp": lax.rem(tp + other, 4)}, device_id_type=MESH)

    vt_s[:, HEAD:, :] = jnp.ones((heads, PAD, 4 * own), vt_s.dtype)

    def near(i):
        rows = pl.ds(_aligned(mine + i * HALF, HALF), HALF)
        return remote(xn_s.at[rows, :], xn_s.at[rows, :], near_send.at[i], near_recv.at[i], mate)

    def near_in(i):
        rows = pl.ds(_aligned(mates + i * HALF, HALF), HALF)
        return remote(xn_s.at[rows, :], xn_s.at[rows, :], near_send.at[i], near_recv.at[i], mate)

    def far(s):
        rows = pl.ds(_aligned(here + s * BLOCK + c * HALF, HALF), HALF)
        return remote(xn_s.at[rows, :], xn_s.at[rows, :], far_send.at[s], far_recv.at[s], peer)

    def far_in(s):
        rows = pl.ds(_aligned(there + s * BLOCK + c * HALF, HALF), HALF)
        return remote(xn_s.at[rows, :], xn_s.at[rows, :], far_send.at[s], far_recv.at[s], peer)

    def onward(s):
        rows = pl.ds(_aligned(there + s * BLOCK + c * HALF, HALF), HALF)
        return remote(xn_s.at[rows, :], xn_s.at[rows, :], pass_send.at[s], pass_recv.at[s], mate)

    def onward_in(s):
        rows = pl.ds(_aligned(there + s * BLOCK + (1 - c) * HALF, HALF), HALF)
        return remote(xn_s.at[rows, :], xn_s.at[rows, :], pass_send.at[s], pass_recv.at[s], mate)

    def norm(i):
        load_x(i).wait()

        def some(r, _):
            at = _aligned(i * HALF + r * 32, 32)
            wide = x_s[pl.ds(at, 32), :].astype(jnp.float32)
            scale = lax.rsqrt(jnp.mean(wide * wide, -1, keepdims=True) + 1e-6)
            xn_s[pl.ds(_aligned(mine + at, 32), 32), :] = (wide * scale * gain_ref[...].astype(jnp.float32)).astype(xn_s.dtype)
            return _

        lax.fori_loop(0, HALF // 32, some, None)

    norm(0)
    norm(1)
    pl.semaphore_wait(barrier, 3)
    near(0).start()
    near(1).start()

    def first_far(s, sender):
        @pl.when(c != sender)
        def _():
            near_in(2 * (s % 2) + c).wait_recv()

        far(s).start()

    @pl.when(c == 0)
    def _():
        far(0).start()

    norm(2)
    near(2).start()

    @pl.when(c == 0)
    def _():
        far(1).start()

    norm(3)
    near(3).start()

    @pl.when(c == 1)
    def _():
        near_in(1).wait_recv()
        far(0).start()
        near_in(3).wait_recv()
        far(1).start()

    load_wo.wait()
    share_wo = remote(wo_s.at[c], wo_s.at[c], wo_send, wo_recv, mate)
    share_wo_in = remote(wo_s.at[1 - c], wo_s.at[1 - c], wo_send, wo_recv, mate)
    share_wo.start()

    def project(row):
        row = _aligned(row, BLOCK)
        rows = pl.ds(row, BLOCK)
        a = xn_s[rows, :]
        block = lax.div(row, BLOCK)
        cb, sb = cos_at[pl.ds(block, 1), :], sin_at[pl.ds(block, 1), :]
        cos = cb * cos_in[...] - sb * sin_in[...]
        sin = sb * cos_in[...] + cb * sin_in[...]
        for i, to in ((0, q_s), (1, k_s)):
            t = _dot(a, w_s[i], 1, 0).astype(jnp.bfloat16)
            for h in range(heads):
                u = t[:, h * HEAD : (h + 1) * HEAD].astype(jnp.float32)
                to[h, rows, :] = (u * cos + pltpu.roll(u, HEAD // 2, 1) * sin).astype(to.dtype)
        t = _dot(a, w_s[2], 1, 0).astype(jnp.bfloat16)
        for h in range(heads):
            vt_s[h, :HEAD, rows] = t[:, h * HEAD : (h + 1) * HEAD].T

    e = HEAD**-0.5 * LOG2E

    def attend(row):
        row = _aligned(row, BLOCK)
        rows = pl.ds(row, BLOCK)
        top_s[...] = jnp.full(top_s.shape, NEG, jnp.float32)
        mix_s[...] = jnp.zeros(mix_s.shape, jnp.float32)

        def step(j, masked):
            keys = pl.ds(_aligned(j * BLOCK, BLOCK), BLOCK)
            scores = [_dot(k_s[h, keys, :], q_s[h, rows, :], 1, 1) for h in range(heads)]
            weights, keeps = [], []
            if masked:
                ok = lax.broadcasted_iota(jnp.int32, (BLOCK, BLOCK), 1) >= lax.broadcasted_iota(jnp.int32, (BLOCK, BLOCK), 0)
            for h, s in enumerate(scores):
                if masked:
                    s = jnp.where(ok, s, HIDDEN)
                old = top_s[h : h + 1, :]
                top = jnp.maximum(old, s.max(axis=0, keepdims=True))
                top_s[h : h + 1, :] = top
                weights.append(jnp.exp2((s - top) * e).astype(jnp.bfloat16))
                keeps.append(jnp.exp2((old - top) * e))
            for h, (p, keep) in enumerate(zip(weights, keeps)):
                mix_s[h] = mix_s[h] * keep + _dot(vt_s[h, :, keys], p, 1, 0)

        last = lax.div(row, BLOCK)
        lax.fori_loop(0, last, lambda j, _: step(j, False), None)
        step(last, True)
        for h in range(heads):
            out = (mix_s[h, :HEAD, :] * (1 / mix_s[h, HEAD : HEAD + 1, :])).astype(seen_s.dtype)
            seen_s[c, rows, h * HEAD : (h + 1) * HEAD] = out.T

    def seen_out(s):
        rows = pl.ds(_aligned(there + s * BLOCK + (1 - c) * HALF, HALF), HALF)
        return remote(seen_s.at[c, rows, :], seen_s.at[c, rows, :], seen_send.at[s], seen_recv.at[s], mate)

    def seen_in(s):
        rows = pl.ds(_aligned(there + s * BLOCK + c * HALF, HALF), HALF)
        return remote(seen_s.at[1 - c, rows, :], seen_s.at[1 - c, rows, :], seen_send.at[s], seen_recv.at[s], mate)

    def term_out(s):
        j = 2 * lax.rem(s, 2) + c
        src = term_s.at[pl.ds(_aligned(s * HALF, HALF), HALF), :]
        dst = got_s.at[pl.ds(_aligned(j * HALF, HALF), HALF), :]
        return remote(src, dst, term_send.at[s], term_recv.at[j], 2 * (1 - chip) + lax.div(s, 2))

    def term(s):
        seen_in(s).wait_recv()
        rows = pl.ds(_aligned(there + s * BLOCK + c * HALF, HALF), HALF)
        a, b = seen_s[0, rows, :], seen_s[1, rows, :]
        for n in range(0, width, 512):
            t = _dot(a, wo_s[0, :, n : n + 512], 1, 0) + _dot(b, wo_s[1, :, n : n + 512], 1, 0)
            term_s[pl.ds(_aligned(s * HALF, HALF), HALF), n : n + 512] = t.astype(term_s.dtype)
        term_out(s).start()

    for i in range(3):
        load_w(i).wait()
    project(mine)

    for s in (2, 3):

        @pl.when(c == 0)
        def _():
            near_in(2 * (s - 2)).wait_recv()

        far(s).start()

    near_in(1 - c).wait_recv()
    near_in(3 - c).wait_recv()

    def local(i, _):
        at = lax.rem(2 * c + 1 + i, 4)
        project(here + at * BLOCK)
        return _

    lax.fori_loop(0, 3, local, None)
    share_wo_in.wait_recv()

    def arrived(s, _):
        far_in(s).wait_recv()
        onward(s).start()

        @pl.when(s > 0)
        def _():
            term(s - 1)

        onward_in(s).wait_recv()
        project(there + s * BLOCK)
        attend(there + s * BLOCK)
        seen_out(s).start()
        return _

    lax.fori_loop(0, 4, arrived, None)

    def mine_out(i):
        rows = pl.ds(_aligned(mates + i * BLOCK, BLOCK), BLOCK)
        return remote(seen_s.at[c, rows, :], seen_s.at[c, rows, :], mine_send.at[i], mine_recv.at[i], mate)

    def mine_in(i):
        rows = pl.ds(_aligned(mine + i * BLOCK, BLOCK), BLOCK)
        return remote(seen_s.at[1 - c, rows, :], seen_s.at[1 - c, rows, :], mine_send.at[i], mine_recv.at[i], mate)

    def inside(i, _):
        at = lax.rem(2 * (1 - c) + i, 4)
        attend(here + at * BLOCK)

        @pl.when(i == 0)
        def _():
            term(3)

        @pl.when(i < 2)
        def _():
            mine_out(i).start()

        return _

    lax.fori_loop(0, 4, inside, None)

    def keep(i, _):
        mine_in(i).wait_recv()
        rows = pl.ds(_aligned(mine + i * BLOCK, BLOCK), BLOCK)
        to = pl.ds(_aligned(i * BLOCK, BLOCK), BLOCK)
        a, b = seen_s[0, rows, :], seen_s[1, rows, :]
        for n in range(0, width, 512):
            t = _dot(a, wo_s[0, :, n : n + 512], 1, 0) + _dot(b, wo_s[1, :, n : n + 512], 1, 0)
            acc_s[to, n : n + 512] = t + x_s[to, n : n + 512].astype(jnp.float32)
        return _

    lax.fori_loop(0, 2, keep, None)

    def term_in(j):
        rows = pl.ds(j * HALF, HALF)
        return remote(got_s.at[rows, :], got_s.at[rows, :], term_send.at[j], term_recv.at[j], peer)

    def put(j):
        rows = pl.ds(j * HALF, HALF)
        return pltpu.make_async_copy(y_s.at[rows, :], y_hbm.at[rows, :], out_sem.at[j])

    for j in range(4):
        term_in(j).wait_recv()

        def add(r, _):
            rows = pl.ds(_aligned(j * HALF + r * 32, 32), 32)
            y_s[rows, :] = (acc_s[rows, :] + got_s[rows, :].astype(jnp.float32)).astype(y_s.dtype)
            return _

        lax.fori_loop(0, HALF // 32, add, None)
        put(j).start()

    for s in range(4):
        near(s).wait_send()
        far(s).wait_send()
        onward(s).wait_send()
        seen_out(s).wait_send()
        term_out(s).wait_send()
    for i in range(2):
        mine_out(i).wait_send()
    share_wo.wait_send()
    for j in range(4):
        put(j).wait()


def _tables(tokens):
    half = HEAD // 2
    rate = np.float32(THETA) ** (-np.arange(half, dtype=np.float32) / np.float32(half))
    sign = np.concatenate([-np.ones(half), np.ones(half)])

    def pair(place):
        angle = place[:, None].astype(np.float64) * np.tile(rate, 2).astype(np.float64)
        return np.cos(angle).astype(np.float32), (np.sin(angle) * sign).astype(np.float32)

    return *pair(np.arange(BLOCK)), *pair(np.arange(0, tokens, BLOCK))


def solution(mesh):
    def step(x, gain, wq, wk, wv, wo):
        own, width = x.shape
        tokens = 4 * own
        inner = wq.shape[1]
        heads = inner // HEAD
        low = jnp.bfloat16
        dma = pltpu.SemaphoreType.DMA
        hbm = pl.BlockSpec(memory_space=pl.ANY)
        vmem = pl.BlockSpec(memory_space=pltpu.VMEM)
        return pl.pallas_call(
            functools.partial(kernel, own),
            name="layer",
            out_shape=jax.ShapeDtypeStruct((own, width), low),
            in_specs=[hbm, vmem, hbm, hbm, hbm, hbm, vmem, vmem, vmem, vmem],
            out_specs=hbm,
            scratch_shapes=[
                pltpu.VMEM((own, width), low),
                pltpu.VMEM((tokens, width), low),
                pltpu.VMEM((3, width, inner), low),
                pltpu.VMEM((2, inner, width), low),
                pltpu.VMEM((heads, tokens, HEAD), low),
                pltpu.VMEM((heads, tokens, HEAD), low),
                pltpu.VMEM((heads, HEAD + PAD, tokens), low),
                pltpu.VMEM((2, tokens, inner), low),
                pltpu.VMEM((8, BLOCK), jnp.float32),
                pltpu.VMEM((heads, HEAD + PAD, BLOCK), jnp.float32),
                pltpu.VMEM((own, width), low),
                pltpu.VMEM((own, width), low),
                pltpu.VMEM((own, width), jnp.float32),
                pltpu.VMEM((own, width), low),
                dma((8,)), dma((4,)), dma((4,)), dma((4,)), dma((4,)), dma((4,)), dma((4,)), dma((4,)),
                dma((4,)), dma((4,)), dma((2,)), dma((2,)), dma, dma, dma((4,)), dma((4,)),
            ],
            compiler_params=pltpu.CompilerParams(collective_id=0, has_side_effects=True, vmem_limit_bytes=67043328),
        )(x, gain.reshape(1, width), wq, wk, wv, wo, *(jnp.asarray(t) for t in _tables(tokens)))

    tokens, columns = P(("dp", "tp"), None), P(None, "tp")
    return jax.shard_map(
        step,
        mesh=mesh,
        in_specs=(tokens, P(None), columns, columns, columns, P("tp", None)),
        out_specs=tokens,
        check_vma=False,
    )
```

```python
import functools

import jax
import jax.numpy as jnp
import numpy as np
from jax import lax
from jax.experimental import pallas as pl
from jax.experimental.pallas import tpu as pltpu
from jax.sharding import PartitionSpec as P

HEAD = 128
THETA = 10000
VMEM = 60 * 2**20
NEG = -1e30
HIDDEN = 2 * NEG
LOG2E = 1.4426950408889634
MESH = pl.DeviceIdType.MESH
BLOCK = 256
HALF = BLOCK // 2
PIECES = 4
PIECE = HALF // PIECES
PAD = 16


def _dot(a, b, ca, cb):
    return lax.dot_general(a, b, (((ca,), (cb,)), ((), ())), preferred_element_type=jnp.float32)


def _aligned(x, n):
    return pl.multiple_of(x, n)


def kernel(own, x_hbm, gain_hbm, wq_hbm, wk_hbm, wv_hbm, wo_hbm, turn_hbm, y_ref,
           x_s, gain_s, turn_s, xn_s, w_s, wo_s, q_s, k_s, vt_s, seen_s, top_s, mix_s, term_s, got_s, acc_s,
           load_sem, near_send, near_recv, lead_send, lead_recv, far_send, far_recv, pass_send, pass_recv,
           seen_send, seen_recv, mine_send, mine_recv, wo_send, wo_recv, term_send, term_recv,
           last_send, last_recv):
    heads = q_s.shape[0]
    width = x_s.shape[1]
    inner = heads * HEAD
    tp = lax.axis_index("tp")
    c = lax.rem(tp, 2)
    chip = lax.div(tp, 2)
    mate = tp + 1 - 2 * c
    peer = lax.rem(tp + 2, 4)
    here = chip * (2 * own)
    there = (1 - chip) * (2 * own)
    mine = here + c * own
    mates = here + (1 - c) * own

    def remote(src, dst, send, recv, device):
        return pltpu.make_async_remote_copy(src_ref=src, dst_ref=dst, send_sem=send, recv_sem=recv, device_id={"tp": device}, device_id_type=MESH)

    def load_x(i):
        rows = pl.ds(i * PIECE, PIECE) if i < PIECES else pl.ds((i - PIECES + 1) * HALF, HALF)
        return pltpu.make_async_copy(x_hbm.at[rows, :], x_s.at[rows, :], load_sem.at[i])

    def load_w(i):
        return pltpu.make_async_copy((wq_hbm, wk_hbm, wv_hbm)[i], w_s.at[i], load_sem.at[PIECES + 3 + i])

    load_wo = pltpu.make_async_copy(wo_hbm, wo_s.at[c], load_sem.at[PIECES + 6])
    load_gain = pltpu.make_async_copy(gain_hbm, gain_s, load_sem.at[PIECES + 7])
    load_turn = pltpu.make_async_copy(turn_hbm, turn_s, load_sem.at[PIECES + 8])
    load_x(0).start()
    load_gain.start()
    for i in range(1, PIECES + 3):
        load_x(i).start()
    for i in range(3):
        load_w(i).start()
    load_turn.start()
    load_wo.start()

    barrier = pltpu.get_barrier_semaphore()
    for other in range(1, 4):
        pl.semaphore_signal(barrier, inc=1, device_id={"tp": lax.rem(tp + other, 4)}, device_id_type=MESH)

    vt_s[:, HEAD:, :] = jnp.ones((heads, PAD, 4 * own), vt_s.dtype)

    def near(i):
        rows = pl.ds(_aligned(mine + i * HALF, HALF), HALF)
        return remote(xn_s.at[rows, :], xn_s.at[rows, :], near_send.at[i], near_recv.at[i], mate)

    def near_in(i):
        rows = pl.ds(_aligned(mates + i * HALF, HALF), HALF)
        return remote(xn_s.at[rows, :], xn_s.at[rows, :], near_send.at[i], near_recv.at[i], mate)

    def far(s):
        rows = pl.ds(_aligned(here + s * BLOCK + c * HALF, HALF), HALF)
        return remote(xn_s.at[rows, :], xn_s.at[rows, :], far_send.at[s], far_recv.at[s], peer)

    def far_in(s):
        rows = pl.ds(_aligned(there + s * BLOCK + c * HALF, HALF), HALF)
        return remote(xn_s.at[rows, :], xn_s.at[rows, :], far_send.at[s], far_recv.at[s], peer)

    def lead(p):
        rows = pl.ds(_aligned(here + c * HALF + p * PIECE, PIECE), PIECE)
        return remote(xn_s.at[rows, :], xn_s.at[rows, :], lead_send.at[p], lead_recv.at[p], peer)

    def lead_in(p):
        rows = pl.ds(_aligned(there + c * HALF + p * PIECE, PIECE), PIECE)
        return remote(xn_s.at[rows, :], xn_s.at[rows, :], lead_send.at[p], lead_recv.at[p], peer)

    def onward(s):
        rows = pl.ds(_aligned(there + s * BLOCK + c * HALF, HALF), HALF)
        return remote(xn_s.at[rows, :], xn_s.at[rows, :], pass_send.at[s], pass_recv.at[s], mate)

    def onward_in(s):
        rows = pl.ds(_aligned(there + s * BLOCK + (1 - c) * HALF, HALF), HALF)
        return remote(xn_s.at[rows, :], xn_s.at[rows, :], pass_send.at[s], pass_recv.at[s], mate)

    def norm(first, rows):
        def some(r, _):
            at = _aligned(first + r * PIECE, PIECE)
            to = pl.ds(_aligned(mine + at, PIECE), PIECE)
            wide = x_s[pl.ds(at, PIECE), :].astype(jnp.float32)
            scale = lax.rsqrt(jnp.mean(wide * wide, -1, keepdims=True) + 1e-6)
            for g in range(width // 128):
                lanes = slice(g * 128, (g + 1) * 128)
                xn_s[to, lanes] = (wide[:, lanes] * scale * gain_s[g : g + 1, :].astype(jnp.float32)).astype(xn_s.dtype)
            return _

        lax.fori_loop(0, rows // PIECE, some, None)

    for p in range(PIECES):
        load_x(p).wait()
        if p == 0:
            load_gain.wait()
        norm(p * PIECE, PIECE)
        if p == 0:
            pl.semaphore_wait(barrier, 3)

        @pl.when(c == 0)
        def _():
            lead(p).start()

    near(0).start()
    for i in range(1, 4):
        load_x(PIECES - 1 + i).wait()
        norm(i * HALF, HALF)
        near(i).start()
        if i == 2:

            @pl.when(c == 0)
            def _():
                far(1).start()

    @pl.when(c == 1)
    def _():
        near_in(1).wait_recv()
        for p in range(PIECES):
            lead(p).start()
        near_in(3).wait_recv()
        far(1).start()

    load_wo.wait()
    share_wo = remote(wo_s.at[c], wo_s.at[c], wo_send, wo_recv, mate)
    share_wo_in = remote(wo_s.at[1 - c], wo_s.at[1 - c], wo_send, wo_recv, mate)
    share_wo.start()

    def project(row):
        row = _aligned(row, BLOCK)
        rows = pl.ds(row, BLOCK)
        a = xn_s[rows, :]
        block = lax.div(row, BLOCK)
        cos_in, sin_in = turn_s[0, :BLOCK, :], turn_s[1, :BLOCK, :]
        cb, sb = turn_s[0, pl.ds(BLOCK + block, 1), :], turn_s[1, pl.ds(BLOCK + block, 1), :]
        cos = cb * cos_in - sb * sin_in
        sin = sb * cos_in + cb * sin_in
        for i, to in ((0, q_s), (1, k_s)):
            t = _dot(a, w_s[i], 1, 0).astype(jnp.bfloat16)
            for h in range(heads):
                u = t[:, h * HEAD : (h + 1) * HEAD].astype(jnp.float32)
                to[h, rows, :] = (u * cos + pltpu.roll(u, HEAD // 2, 1) * sin).astype(to.dtype)
        t = _dot(a, w_s[2], 1, 0).astype(jnp.bfloat16)
        for h in range(heads):
            vt_s[h, :HEAD, rows] = t[:, h * HEAD : (h + 1) * HEAD].T

    e = HEAD**-0.5 * LOG2E

    def attend(row):
        row = _aligned(row, BLOCK)
        rows = pl.ds(row, BLOCK)
        top_s[...] = jnp.full(top_s.shape, NEG, jnp.float32)
        mix_s[...] = jnp.zeros(mix_s.shape, jnp.float32)

        def step(j, masked):
            keys = pl.ds(_aligned(j * BLOCK, BLOCK), BLOCK)
            scores = [_dot(k_s[h, keys, :], q_s[h, rows, :], 1, 1) for h in range(heads)]
            weights, keeps = [], []
            if masked:
                ok = lax.broadcasted_iota(jnp.int32, (BLOCK, BLOCK), 1) >= lax.broadcasted_iota(jnp.int32, (BLOCK, BLOCK), 0)
            for h, s in enumerate(scores):
                if masked:
                    s = jnp.where(ok, s, HIDDEN)
                old = top_s[h : h + 1, :]
                top = jnp.maximum(old, s.max(axis=0, keepdims=True))
                top_s[h : h + 1, :] = top
                weights.append(jnp.exp2((s - top) * e).astype(jnp.bfloat16))
                keeps.append(jnp.exp2((old - top) * e))
            for h, (p, keep) in enumerate(zip(weights, keeps)):
                mix_s[h] = mix_s[h] * keep + _dot(vt_s[h, :, keys], p, 1, 0)

        last = lax.div(row, BLOCK)
        lax.fori_loop(0, last, lambda j, _: step(j, False), None)
        step(last, True)
        for h in range(heads):
            out = (mix_s[h, :HEAD, :] * (1 / mix_s[h, HEAD : HEAD + 1, :])).astype(seen_s.dtype)
            seen_s[c, rows, h * HEAD : (h + 1) * HEAD] = out.T

    def seen_out(s):
        rows = pl.ds(_aligned(there + s * BLOCK + (1 - c) * HALF, HALF), HALF)
        return remote(seen_s.at[c, rows, :], seen_s.at[c, rows, :], seen_send.at[s], seen_recv.at[s], mate)

    def seen_in(s):
        rows = pl.ds(_aligned(there + s * BLOCK + c * HALF, HALF), HALF)
        return remote(seen_s.at[1 - c, rows, :], seen_s.at[1 - c, rows, :], seen_send.at[s], seen_recv.at[s], mate)

    def term_out(s):
        j = 2 * lax.rem(s, 2) + c
        src = term_s.at[pl.ds(_aligned(s * HALF, HALF), HALF), :]
        dst = got_s.at[pl.ds(_aligned(j * HALF, HALF), HALF), :]
        return remote(src, dst, term_send.at[s], term_recv.at[j], 2 * (1 - chip) + lax.div(s, 2))

    def last_out(p):
        src = term_s.at[pl.ds(3 * HALF + p * PIECE, PIECE), :]
        dst = got_s.at[pl.ds(_aligned((2 + c) * HALF + p * PIECE, PIECE), PIECE), :]
        return remote(src, dst, last_send.at[p], last_recv.at[PIECES * c + p], 2 * (1 - chip) + 1)

    def term(s):
        seen_in(s).wait_recv()
        rows = pl.ds(_aligned(there + s * BLOCK + c * HALF, HALF), HALF)
        a, b = seen_s[0, rows, :], seen_s[1, rows, :]
        for n in range(0, width, 512):
            t = _dot(a, wo_s[0, :, n : n + 512], 1, 0) + _dot(b, wo_s[1, :, n : n + 512], 1, 0)
            term_s[pl.ds(_aligned(s * HALF, HALF), HALF), n : n + 512] = t.astype(term_s.dtype)

    load_turn.wait()
    for i in range(3):
        load_w(i).wait()
    project(mine)

    for s in (2, 3):

        @pl.when(c == 0)
        def _():
            near_in(2 * (s - 2)).wait_recv()

        far(s).start()

    near_in(1 - c).wait_recv()
    near_in(3 - c).wait_recv()

    def local(i, _):
        at = lax.rem(2 * c + 1 + i, 4)
        project(here + at * BLOCK)
        return _

    lax.fori_loop(0, 3, local, None)
    share_wo_in.wait_recv()

    def arrived(s, _):
        @pl.when(s == 0)
        def _():
            for p in range(PIECES):
                lead_in(p).wait_recv()

        @pl.when(s > 0)
        def _():
            far_in(s).wait_recv()

        onward(s).start()

        @pl.when(s > 0)
        def _():
            term(s - 1)
            term_out(s - 1).start()

        onward_in(s).wait_recv()
        project(there + s * BLOCK)
        attend(there + s * BLOCK)
        seen_out(s).start()
        return _

    lax.fori_loop(0, 4, arrived, None)

    def mine_out(i):
        rows = pl.ds(_aligned(mates + i * BLOCK, BLOCK), BLOCK)
        return remote(seen_s.at[c, rows, :], seen_s.at[c, rows, :], mine_send.at[i], mine_recv.at[i], mate)

    def mine_in(i):
        rows = pl.ds(_aligned(mine + i * BLOCK, BLOCK), BLOCK)
        return remote(seen_s.at[1 - c, rows, :], seen_s.at[1 - c, rows, :], mine_send.at[i], mine_recv.at[i], mate)

    def inside(i, _):
        at = lax.rem(2 * (1 - c) + i, 4)
        attend(here + at * BLOCK)

        @pl.when(i == 0)
        def _():
            term(3)
            for p in range(PIECES):
                last_out(p).start()

        @pl.when(i < 2)
        def _():
            mine_out(i).start()

        return _

    lax.fori_loop(0, 4, inside, None)

    def keep(i, _):
        mine_in(i).wait_recv()
        rows = pl.ds(_aligned(mine + i * BLOCK, BLOCK), BLOCK)
        to = pl.ds(_aligned(i * BLOCK, BLOCK), BLOCK)
        a, b = seen_s[0, rows, :], seen_s[1, rows, :]
        for n in range(0, width, 512):
            t = _dot(a, wo_s[0, :, n : n + 512], 1, 0) + _dot(b, wo_s[1, :, n : n + 512], 1, 0)
            acc_s[to, n : n + 512] = t + x_s[to, n : n + 512].astype(jnp.float32)
        return _

    lax.fori_loop(0, 2, keep, None)

    def term_in(j):
        rows = pl.ds(j * HALF, HALF)
        return remote(got_s.at[rows, :], got_s.at[rows, :], term_send.at[0], term_recv.at[j], peer)

    def last_in(j, p):
        rows = pl.ds((2 + j) * HALF + p * PIECE, PIECE)
        return remote(got_s.at[rows, :], got_s.at[rows, :], last_send.at[p], last_recv.at[PIECES * j + p], peer)

    def finish(first, rows):
        def some(r, _):
            at = pl.ds(_aligned(first + r * PIECE, PIECE), PIECE)
            y_ref[at, :] = (acc_s[at, :] + got_s[at, :].astype(jnp.float32)).astype(y_ref.dtype)
            return _

        lax.fori_loop(0, rows // PIECE, some, None)

    for j in range(2):
        term_in(j).wait_recv()
        finish(j * HALF, HALF)

    @pl.when(c == 0)
    def _():
        for j in range(2, 4):
            term_in(j).wait_recv()
            finish(j * HALF, HALF)

    @pl.when(c == 1)
    def _():
        for p in range(PIECES):
            for j in range(2):
                last_in(j, p).wait_recv()
                finish((2 + j) * HALF + p * PIECE, PIECE)

    for s in range(4):
        near(s).wait_send()
        onward(s).wait_send()
        seen_out(s).wait_send()
        if s > 0:
            far(s).wait_send()
        if s < 3:
            term_out(s).wait_send()
    for p in range(PIECES):
        lead(p).wait_send()
        last_out(p).wait_send()
    for i in range(2):
        mine_out(i).wait_send()
    share_wo.wait_send()


def _tables(tokens):
    half = HEAD // 2
    rate = np.float32(THETA) ** (-np.arange(half, dtype=np.float32) / np.float32(half))
    sign = np.concatenate([-np.ones(half), np.ones(half)])

    def pair(place):
        angle = place[:, None].astype(np.float64) * np.tile(rate, 2).astype(np.float64)
        return np.cos(angle).astype(np.float32), (np.sin(angle) * sign).astype(np.float32)

    both = zip(pair(np.arange(BLOCK)), pair(np.arange(0, tokens, BLOCK)))
    return np.stack([np.concatenate(t) for t in both])


def solution(mesh):
    def step(x, gain, wq, wk, wv, wo):
        own, width = x.shape
        tokens = 4 * own
        inner = wq.shape[1]
        heads = inner // HEAD
        low = jnp.bfloat16
        dma = pltpu.SemaphoreType.DMA
        hbm = pl.BlockSpec(memory_space=pl.ANY)
        return pl.pallas_call(
            functools.partial(kernel, own),
            name="layer",
            out_shape=pltpu.VMEM((own, width), low),
            in_specs=[hbm] * 7,
            out_specs=pl.BlockSpec(memory_space=pltpu.VMEM),
            scratch_shapes=[
                pltpu.VMEM((own, width), low),
                pltpu.VMEM((width // 128, 128), low),
                pltpu.VMEM((2, BLOCK + tokens // BLOCK, HEAD), jnp.float32),
                pltpu.VMEM((tokens, width), low),
                pltpu.VMEM((3, width, inner), low),
                pltpu.VMEM((2, inner, width), low),
                pltpu.VMEM((heads, tokens, HEAD), low),
                pltpu.VMEM((heads, tokens, HEAD), low),
                pltpu.VMEM((heads, HEAD + PAD, tokens), low),
                pltpu.VMEM((2, tokens, inner), low),
                pltpu.VMEM((8, BLOCK), jnp.float32),
                pltpu.VMEM((heads, HEAD + PAD, BLOCK), jnp.float32),
                pltpu.VMEM((own, width), low),
                pltpu.VMEM((own, width), low),
                pltpu.VMEM((own, width), jnp.float32),
                dma((PIECES + 9,)), dma((4,)), dma((4,)), dma((PIECES,)), dma((PIECES,)), dma((4,)), dma((4,)), dma((4,)), dma((4,)),
                dma((4,)), dma((4,)), dma((2,)), dma((2,)), dma, dma, dma((4,)), dma((4,)), dma((PIECES,)), dma((2 * PIECES,)),
            ],
            compiler_params=pltpu.CompilerParams(collective_id=0, has_side_effects=True, vmem_limit_bytes=VMEM),
        )(x, gain.reshape(width // 128, 128), wq, wk, wv, wo, jnp.asarray(_tables(tokens)))

    tokens, columns = P(("dp", "tp"), None), P(None, "tp")
    return jax.shard_map(
        step,
        mesh=mesh,
        in_specs=(tokens, P(None), columns, columns, columns, P("tp", None)),
        out_specs=tokens,
        check_vma=False,
    )
```

```python
import functools

import jax
import jax.numpy as jnp
import numpy as np
from jax import lax
from jax.experimental import pallas as pl
from jax.experimental.pallas import tpu as pltpu
from jax.sharding import PartitionSpec as P

HEAD = 128
THETA = 10000
VMEM = 60 * 2**20
NEG = float(np.finfo(np.float32).min)
HIDDEN = -np.inf
LOG2E = 1.4426950408889634
MESH = pl.DeviceIdType.MESH
BLOCK = 256
HALF = BLOCK // 2
QUARTER = HALF // 2
PIECES = 4
PIECE = HALF // PIECES
PAD = 16


def _dot(a, b, ca, cb):
    return lax.dot_general(a, b, (((ca,), (cb,)), ((), ())), preferred_element_type=jnp.float32)


def _aligned(x, n):
    return pl.multiple_of(x, n)


def kernel(own, x_hbm, gain_hbm, wq_hbm, wk_hbm, wv_hbm, wo_hbm, turn_hbm, y_ref,
           x_s, gain_s, turn_s, xn_s, w_s, wo_s, q_s, k_s, vt_s, seen_s, top_s, mix_s, term_s, got_s, acc_s,
           load_sem, near_send, near_recv, far_send, far_recv, pass_send, pass_recv,
           seen_send, seen_recv, mine_send, mine_recv, wo_send, wo_recv, term_send, term_recv,
           last_send, last_recv):
    heads = q_s.shape[0]
    width = x_s.shape[1]
    inner = heads * HEAD
    tp = lax.axis_index("tp")
    c = lax.rem(tp, 2)
    chip = lax.div(tp, 2)
    mate = tp + 1 - 2 * c
    peer = lax.rem(tp + 2, 4)
    here = chip * (2 * own)
    there = (1 - chip) * (2 * own)
    mine = here + c * own
    mates = here + (1 - c) * own

    def remote(src, dst, send, recv, device):
        return pltpu.make_async_remote_copy(src_ref=src, dst_ref=dst, send_sem=send, recv_sem=recv, device_id={"tp": device}, device_id_type=MESH)

    def load_x(i):
        rows = pl.ds(_aligned(i * QUARTER, QUARTER), QUARTER)
        return pltpu.make_async_copy(x_hbm.at[rows, :], x_s.at[rows, :], load_sem.at[i])

    def load_w(i):
        return pltpu.make_async_copy((wq_hbm, wk_hbm, wv_hbm)[i], w_s.at[i], load_sem.at[8 + i])

    load_wo = pltpu.make_async_copy(wo_hbm, wo_s.at[c], load_sem.at[11])
    load_gain = pltpu.make_async_copy(gain_hbm, gain_s, load_sem.at[12])
    load_turn = pltpu.make_async_copy(turn_hbm, turn_s, load_sem.at[13])
    order = [lax.rem(2 * c + j, 8) for j in range(8)]
    load_x(order[0]).start()
    load_gain.start()
    for i in order[1:]:
        load_x(i).start()
    for i in range(3):
        load_w(i).start()
    load_turn.start()
    load_wo.start()

    barrier = pltpu.get_barrier_semaphore()
    for other in range(1, 4):
        pl.semaphore_signal(barrier, inc=1, device_id={"tp": lax.rem(tp + other, 4)}, device_id_type=MESH)

    vt_s[:, HEAD:, :] = jnp.ones((heads, PAD, 4 * own), vt_s.dtype)

    def near(i):
        rows = pl.ds(_aligned(mine + i * HALF, HALF), HALF)
        return remote(xn_s.at[rows, :], xn_s.at[rows, :], near_send.at[i], near_recv.at[i], mate)

    def near_in(i):
        rows = pl.ds(_aligned(mates + i * HALF, HALF), HALF)
        return remote(xn_s.at[rows, :], xn_s.at[rows, :], near_send.at[i], near_recv.at[i], mate)

    def far(k):
        rows = pl.ds(_aligned(here + lax.div(k, 2) * BLOCK + c * HALF + lax.rem(k, 2) * QUARTER, QUARTER), QUARTER)
        return remote(xn_s.at[rows, :], xn_s.at[rows, :], far_send.at[k], far_recv.at[k], peer)

    def far_in(k):
        rows = pl.ds(_aligned(there + lax.div(k, 2) * BLOCK + c * HALF + lax.rem(k, 2) * QUARTER, QUARTER), QUARTER)
        return remote(xn_s.at[rows, :], xn_s.at[rows, :], far_send.at[k], far_recv.at[k], peer)

    def onward(s):
        rows = pl.ds(_aligned(there + s * BLOCK + c * HALF, HALF), HALF)
        return remote(xn_s.at[rows, :], xn_s.at[rows, :], pass_send.at[s], pass_recv.at[s], mate)

    def onward_in(s):
        rows = pl.ds(_aligned(there + s * BLOCK + (1 - c) * HALF, HALF), HALF)
        return remote(xn_s.at[rows, :], xn_s.at[rows, :], pass_send.at[s], pass_recv.at[s], mate)

    def norm(i):
        load_x(i).wait()

        def some(r, _):
            at = _aligned(i * QUARTER + r * 32, 32)
            to = pl.ds(_aligned(mine + at, 32), 32)
            wide = x_s[pl.ds(at, 32), :].astype(jnp.float32)
            scale = lax.rsqrt(jnp.mean(wide * wide, -1, keepdims=True) + 1e-6)
            for g in range(width // 128):
                lanes = slice(g * 128, (g + 1) * 128)
                xn_s[to, lanes] = (wide[:, lanes] * scale * gain_s[g : g + 1, :].astype(jnp.float32)).astype(xn_s.dtype)
            return _

        lax.fori_loop(0, QUARTER // 32, some, None)

    def on_core(n):
        return pl.when(c == n)

    load_gain.wait()
    norm(order[0])
    pl.semaphore_wait(barrier, 3)
    far(4 * c).start()
    for j in range(1, 8):
        norm(order[j])
        if j % 2:
            near(lax.rem(c + j // 2, 4)).start()

        @on_core(0)
        def _():
            if j == 1:
                far(1).start()
            if j == 5:
                far(2).start()
                far(3).start()

    @on_core(1)
    def _():
        near_in(1).wait_recv()
        far(0).start()
        far(1).start()
        near_in(3).wait_recv()
        far(2).start()
        far(3).start()
        for k in range(5, 8):
            far(k).start()

    load_wo.wait()
    share_wo = remote(wo_s.at[c], wo_s.at[c], wo_send, wo_recv, mate)
    share_wo_in = remote(wo_s.at[1 - c], wo_s.at[1 - c], wo_send, wo_recv, mate)
    share_wo.start()

    def project(row):
        row = _aligned(row, BLOCK)
        rows = pl.ds(row, BLOCK)
        a = xn_s[rows, :]
        block = lax.div(row, BLOCK)
        cos_in, sin_in = turn_s[0, :BLOCK, :], turn_s[1, :BLOCK, :]
        cb, sb = turn_s[0, pl.ds(BLOCK + block, 1), :], turn_s[1, pl.ds(BLOCK + block, 1), :]
        cos = cb * cos_in - sb * sin_in
        sin = sb * cos_in + cb * sin_in
        for i, to in ((0, q_s), (1, k_s)):
            t = _dot(a, w_s[i], 1, 0).astype(jnp.bfloat16)
            for h in range(heads):
                u = t[:, h * HEAD : (h + 1) * HEAD].astype(jnp.float32)
                to[h, rows, :] = (u * cos + pltpu.roll(u, HEAD // 2, 1) * sin).astype(to.dtype)
        t = _dot(a, w_s[2], 1, 0).astype(jnp.bfloat16)
        for h in range(heads):
            vt_s[h, :HEAD, rows] = t[:, h * HEAD : (h + 1) * HEAD].T

    e = HEAD**-0.5 * LOG2E

    def attend(row):
        row = _aligned(row, BLOCK)
        rows = pl.ds(row, BLOCK)
        top_s[...] = jnp.full(top_s.shape, NEG, jnp.float32)
        mix_s[...] = jnp.zeros(mix_s.shape, jnp.float32)

        def step(j, masked):
            keys = pl.ds(_aligned(j * BLOCK, BLOCK), BLOCK)
            scores = [_dot(k_s[h, keys, :], q_s[h, rows, :], 1, 1) for h in range(heads)]
            weights, keeps = [], []
            if masked:
                ok = lax.broadcasted_iota(jnp.int32, (BLOCK, BLOCK), 1) >= lax.broadcasted_iota(jnp.int32, (BLOCK, BLOCK), 0)
            for h, s in enumerate(scores):
                if masked:
                    s = jnp.where(ok, s, HIDDEN)
                old = top_s[h : h + 1, :]
                top = jnp.maximum(old, s.max(axis=0, keepdims=True))
                top_s[h : h + 1, :] = top
                weights.append(jnp.exp2((s - top) * e).astype(jnp.bfloat16))
                keeps.append(jnp.exp2((old - top) * e))
            for h, (p, keep) in enumerate(zip(weights, keeps)):
                mix_s[h] = mix_s[h] * keep + _dot(vt_s[h, :, keys], p, 1, 0)

        last = lax.div(row, BLOCK)
        lax.fori_loop(0, last, lambda j, _: step(j, False), None)
        step(last, True)
        for h in range(heads):
            out = (mix_s[h, :HEAD, :] * (1 / mix_s[h, HEAD : HEAD + 1, :])).astype(seen_s.dtype)
            seen_s[c, rows, h * HEAD : (h + 1) * HEAD] = out.T

    def seen_out(s):
        rows = pl.ds(_aligned(there + s * BLOCK + (1 - c) * HALF, HALF), HALF)
        return remote(seen_s.at[c, rows, :], seen_s.at[c, rows, :], seen_send.at[s], seen_recv.at[s], mate)

    def seen_in(s):
        rows = pl.ds(_aligned(there + s * BLOCK + c * HALF, HALF), HALF)
        return remote(seen_s.at[1 - c, rows, :], seen_s.at[1 - c, rows, :], seen_send.at[s], seen_recv.at[s], mate)

    def term_out(s):
        j = 2 * lax.rem(s, 2) + c
        src = term_s.at[pl.ds(_aligned(s * HALF, HALF), HALF), :]
        dst = got_s.at[pl.ds(_aligned(j * HALF, HALF), HALF), :]
        return remote(src, dst, term_send.at[s], term_recv.at[j], 2 * (1 - chip) + lax.div(s, 2))

    def last_out(p):
        src = term_s.at[pl.ds(3 * HALF + p * PIECE, PIECE), :]
        dst = got_s.at[pl.ds(_aligned((2 + c) * HALF + p * PIECE, PIECE), PIECE), :]
        return remote(src, dst, last_send.at[p], last_recv.at[PIECES * c + p], 2 * (1 - chip) + 1)

    def term(s):
        seen_in(s).wait_recv()
        rows = pl.ds(_aligned(there + s * BLOCK + c * HALF, HALF), HALF)
        a, b = seen_s[0, rows, :], seen_s[1, rows, :]
        for n in range(0, width, 512):
            t = _dot(a, wo_s[0, :, n : n + 512], 1, 0) + _dot(b, wo_s[1, :, n : n + 512], 1, 0)
            term_s[pl.ds(_aligned(s * HALF, HALF), HALF), n : n + 512] = t.astype(term_s.dtype)

    load_turn.wait()
    for i in range(3):
        load_w(i).wait()
    project(mine)

    @on_core(0)
    def _():
        near_in(0).wait_recv()
        far(4).start()
        far(5).start()
        near_in(2).wait_recv()
        far(6).start()
        far(7).start()

    near_in(1 - c).wait_recv()
    near_in(3 - c).wait_recv()

    def local(i, _):
        at = lax.rem(2 * c + 1 + i, 4)
        project(here + at * BLOCK)
        return _

    lax.fori_loop(0, 3, local, None)
    share_wo_in.wait_recv()

    def arrived(s, _):
        far_in(2 * s).wait_recv()
        far_in(2 * s + 1).wait_recv()
        onward(s).start()

        @pl.when(s > 0)
        def _():
            term(s - 1)
            term_out(s - 1).start()

        onward_in(s).wait_recv()
        project(there + s * BLOCK)
        attend(there + s * BLOCK)
        seen_out(s).start()
        return _

    lax.fori_loop(0, 4, arrived, None)

    def mine_out(i):
        rows = pl.ds(_aligned(mates + i * BLOCK, BLOCK), BLOCK)
        return remote(seen_s.at[c, rows, :], seen_s.at[c, rows, :], mine_send.at[i], mine_recv.at[i], mate)

    def mine_in(i):
        rows = pl.ds(_aligned(mine + i * BLOCK, BLOCK), BLOCK)
        return remote(seen_s.at[1 - c, rows, :], seen_s.at[1 - c, rows, :], mine_send.at[i], mine_recv.at[i], mate)

    def inside(i, _):
        at = lax.rem(2 * (1 - c) + i, 4)
        attend(here + at * BLOCK)

        @pl.when(i == 0)
        def _():
            term(3)
            for p in range(PIECES):
                last_out(p).start()

        @pl.when(i < 2)
        def _():
            mine_out(i).start()

        return _

    lax.fori_loop(0, 4, inside, None)

    def keep(i, _):
        mine_in(i).wait_recv()
        rows = pl.ds(_aligned(mine + i * BLOCK, BLOCK), BLOCK)
        to = pl.ds(_aligned(i * BLOCK, BLOCK), BLOCK)
        a, b = seen_s[0, rows, :], seen_s[1, rows, :]
        for n in range(0, width, 512):
            t = _dot(a, wo_s[0, :, n : n + 512], 1, 0) + _dot(b, wo_s[1, :, n : n + 512], 1, 0)
            acc_s[to, n : n + 512] = t + x_s[to, n : n + 512].astype(jnp.float32)
        return _

    lax.fori_loop(0, 2, keep, None)

    def term_in(j):
        rows = pl.ds(j * HALF, HALF)
        return remote(got_s.at[rows, :], got_s.at[rows, :], term_send.at[0], term_recv.at[j], peer)

    def last_in(j, p):
        rows = pl.ds((2 + j) * HALF + p * PIECE, PIECE)
        return remote(got_s.at[rows, :], got_s.at[rows, :], last_send.at[p], last_recv.at[PIECES * j + p], peer)

    def finish(first, rows):
        def some(r, _):
            at = pl.ds(_aligned(first + r * PIECE, PIECE), PIECE)
            y_ref[at, :] = (acc_s[at, :] + got_s[at, :].astype(jnp.float32)).astype(y_ref.dtype)
            return _

        lax.fori_loop(0, rows // PIECE, some, None)

    for j in range(2):
        term_in(j).wait_recv()
        finish(j * HALF, HALF)

    @pl.when(c == 0)
    def _():
        for j in range(2, 4):
            term_in(j).wait_recv()
            finish(j * HALF, HALF)

    @pl.when(c == 1)
    def _():
        for p in range(PIECES):
            for j in range(2):
                last_in(j, p).wait_recv()
                finish((2 + j) * HALF + p * PIECE, PIECE)

    for s in range(4):
        near(s).wait_send()
        onward(s).wait_send()
        seen_out(s).wait_send()
        far(2 * s).wait_send()
        far(2 * s + 1).wait_send()
        if s < 3:
            term_out(s).wait_send()
    for p in range(PIECES):
        last_out(p).wait_send()
    for i in range(2):
        mine_out(i).wait_send()
    share_wo.wait_send()


def _tables(tokens):
    half = HEAD // 2
    rate = np.float32(THETA) ** (-np.arange(half, dtype=np.float32) / np.float32(half))
    sign = np.concatenate([-np.ones(half), np.ones(half)])

    def pair(place):
        angle = place[:, None].astype(np.float64) * np.tile(rate, 2).astype(np.float64)
        return np.cos(angle).astype(np.float32), (np.sin(angle) * sign).astype(np.float32)

    both = zip(pair(np.arange(BLOCK)), pair(np.arange(0, tokens, BLOCK)))
    return np.stack([np.concatenate(t) for t in both])


def solution(mesh):
    def step(x, gain, wq, wk, wv, wo):
        own, width = x.shape
        tokens = 4 * own
        inner = wq.shape[1]
        heads = inner // HEAD
        low = jnp.bfloat16
        dma = pltpu.SemaphoreType.DMA
        hbm = pl.BlockSpec(memory_space=pl.ANY)
        return pl.pallas_call(
            functools.partial(kernel, own),
            name="layer",
            out_shape=pltpu.VMEM((own, width), low),
            in_specs=[hbm] * 7,
            out_specs=pl.BlockSpec(memory_space=pltpu.VMEM),
            scratch_shapes=[
                pltpu.VMEM((own, width), low),
                pltpu.VMEM((width // 128, 128), low),
                pltpu.VMEM((2, BLOCK + tokens // BLOCK, HEAD), jnp.float32),
                pltpu.VMEM((tokens, width), low),
                pltpu.VMEM((3, width, inner), low),
                pltpu.VMEM((2, inner, width), low),
                pltpu.VMEM((heads, tokens, HEAD), low),
                pltpu.VMEM((heads, tokens, HEAD), low),
                pltpu.VMEM((heads, HEAD + PAD, tokens), low),
                pltpu.VMEM((2, tokens, inner), low),
                pltpu.VMEM((8, BLOCK), jnp.float32),
                pltpu.VMEM((heads, HEAD + PAD, BLOCK), jnp.float32),
                pltpu.VMEM((own, width), low),
                pltpu.VMEM((own, width), low),
                pltpu.VMEM((own, width), jnp.float32),
                dma((14,)), dma((4,)), dma((4,)), dma((8,)), dma((8,)), dma((4,)), dma((4,)), dma((4,)),
                dma((4,)), dma((2,)), dma((2,)), dma, dma, dma((4,)), dma((4,)), dma((PIECES,)), dma((2 * PIECES,)),
            ],
            compiler_params=pltpu.CompilerParams(collective_id=0, has_side_effects=True, vmem_limit_bytes=VMEM),
        )(x, gain.reshape(width // 128, 128), wq, wk, wv, wo, jnp.asarray(_tables(tokens)))

    tokens, columns = P(("dp", "tp"), None), P(None, "tp")
    return jax.shard_map(
        step,
        mesh=mesh,
        in_specs=(tokens, P(None), columns, columns, columns, P("tp", None)),
        out_specs=tokens,
        check_vma=False,
    )
```

```python
import functools

import jax
import jax.numpy as jnp
import numpy as np
from jax import lax
from jax.experimental import pallas as pl
from jax.experimental.pallas import tpu as pltpu
from jax.sharding import PartitionSpec as P

HEAD = 128
THETA = 10000
VMEM = 60 * 2**20
NEG = float(np.finfo(np.float32).min)
HIDDEN = -np.inf
LOG2E = 1.4426950408889634
MESH = pl.DeviceIdType.MESH
BLOCK = 256
HALF = BLOCK // 2
LEAD = 32
LAST = (0, 96), (96, 32)
PAD = 16


def _dot(a, b, ca, cb):
    return lax.dot_general(a, b, (((ca,), (cb,)), ((), ())), preferred_element_type=jnp.float32)


def _aligned(x, n):
    return pl.multiple_of(x, n)


def kernel(own, x_hbm, gain_hbm, wq_hbm, wk_hbm, wv_hbm, wo_hbm, turn_hbm, y_ref,
           x_s, gain_s, turn_s, xn_s, w_s, wo_s, q_s, k_s, vt_s, seen_s, top_s, mix_s, term_s, got_s, acc_s,
           load_sem, mate_sem, row_send, seen_send, wo_send, near_recv, far_recv, pass_recv, seen_recv, mine_recv, wo_recv, term_recv):
    heads = q_s.shape[0]
    width = x_s.shape[1]
    inner = heads * HEAD
    tp = lax.axis_index("tp")
    c = lax.rem(tp, 2)
    chip = lax.div(tp, 2)
    mate = tp + 1 - 2 * c
    peer = lax.rem(tp + 2, 4)
    here = chip * (2 * own)
    there = (1 - chip) * (2 * own)
    mine = here + c * own
    mates = here + (1 - c) * own

    def remote(src, dst, send, recv, device):
        return pltpu.make_async_remote_copy(src_ref=src, dst_ref=dst, send_sem=send, recv_sem=recv, device_id={"tp": device}, device_id_type=MESH)

    first = c * HALF
    order = [lax.rem(c + i, 4) for i in range(4)]

    def load_x(i, at, rows):
        rows = pl.ds(_aligned(at, LEAD), rows)
        return pltpu.make_async_copy(x_hbm.at[rows, :], x_s.at[rows, :], load_sem.at[i])

    load_lead = load_x(0, first, LEAD)
    load_rest = load_x(1, first + LEAD, HALF - LEAD)
    load_others = [load_x(2, order[i] * HALF, HALF) for i in range(1, 4)]

    def load_w(i):
        return pltpu.make_async_copy((wq_hbm, wk_hbm, wv_hbm)[i], w_s.at[i], load_sem.at[3])

    load_wo = pltpu.make_async_copy(wo_hbm, wo_s.at[c], load_sem.at[4])
    load_gain = pltpu.make_async_copy(gain_hbm, gain_s, load_sem.at[5])
    load_turn = pltpu.make_async_copy(turn_hbm, turn_s, load_sem.at[6])
    load_lead.start()
    load_gain.start()

    def on_core(n):
        return pl.when(c == n)

    barrier = pltpu.get_barrier_semaphore()
    pl.semaphore_signal(barrier, inc=1, device_id={"tp": peer}, device_id_type=MESH)

    @on_core(1)
    def _():
        pl.semaphore_signal(barrier, inc=1, device_id={"tp": mate}, device_id_type=MESH)

    def near_rows(base, i, rows, at):
        rows = pl.ds(_aligned(base + i * HALF, HALF), rows)
        return remote(xn_s.at[rows, :], xn_s.at[rows, :], row_send, near_recv.at[at], mate)

    def near(i):
        return near_rows(mine, i, HALF, jnp.where(lax.rem(i, 2) == 1 - c, lax.div(i, 2), 2))

    def near_in(i):
        return near_rows(mates, 2 * i + c, HALF, i)

    near_others = near_rows(mates, 0, 2 * HALF, 2)

    def cross(base, at, rows, i):
        rows = pl.ds(_aligned(base + c * HALF + at, LEAD), rows)
        return remote(xn_s.at[rows, :], xn_s.at[rows, :], row_send, far_recv.at[i], peer)

    def far(s, base):
        return cross(base, s * BLOCK, HALF, s)

    def lead(base):
        return cross(base, 2 * c * BLOCK, LEAD, 4)

    def rest(base):
        return cross(base, 2 * c * BLOCK + LEAD, HALF - LEAD, 2 * c)

    def onward(s):
        rows = pl.ds(_aligned(there + s * BLOCK + c * HALF, HALF), HALF)
        return remote(xn_s.at[rows, :], xn_s.at[rows, :], row_send, pass_recv.at[s], mate)

    def onward_in(s):
        rows = pl.ds(_aligned(there + s * BLOCK + (1 - c) * HALF, HALF), HALF)
        return remote(xn_s.at[rows, :], xn_s.at[rows, :], row_send, pass_recv.at[s], mate)

    def norm(first, rows):
        def some(r, _):
            at = _aligned(first + r * 32, 32)
            to = pl.ds(_aligned(mine + at, 32), 32)
            wide = x_s[pl.ds(at, 32), :].astype(jnp.float32)
            scale = lax.rsqrt(jnp.mean(wide * wide, -1, keepdims=True) + 1e-6)
            for g in range(width // 128):
                lanes = slice(g * 128, (g + 1) * 128)
                xn_s[to, lanes] = (wide[:, lanes] * scale * gain_s[g : g + 1, :].astype(jnp.float32)).astype(xn_s.dtype)
            return _

        lax.fori_loop(0, rows // 32, some, None)

    def tell_mate():
        pl.semaphore_signal(mate_sem, inc=1, device_id={"tp": mate}, device_id_type=MESH)

    load_gain.wait()
    load_lead.wait()
    norm(first, LEAD)

    @on_core(0)
    def _():
        pl.semaphore_wait(barrier, 2)
        tell_mate()

    @on_core(1)
    def _():
        pl.semaphore_wait(barrier, 1)

    lead(here).start()
    load_rest.start()
    for load in load_others:
        load.start()
    for i in range(3):
        load_w(i).start()
    load_turn.start()
    load_wo.start()
    load_rest.wait()
    norm(first + LEAD, HALF - LEAD)

    @on_core(0)
    def _():
        rest(here).start()

    @on_core(1)
    def _():
        pl.semaphore_wait(mate_sem, 1)
        tell_mate()

    near(order[0]).start()
    load_x(2, 0, 3 * HALF).wait()
    for i in range(1, 4):
        norm(order[i] * HALF, HALF)
        near(order[i]).start()
        if i == 2:

            @on_core(0)
            def _():
                far(1, here).start()

    @on_core(0)
    def _():
        pl.semaphore_wait(mate_sem, 1)

    @on_core(1)
    def _():
        near_in(0).wait_recv()
        far(0, here).start()
        near_in(1).wait_recv()
        far(1, here).start()
        rest(here).start()
        far(3, here).start()

    load_wo.wait()
    share_wo = remote(wo_s.at[c], wo_s.at[c], wo_send, wo_recv, mate)
    share_wo_in = remote(wo_s.at[1 - c], wo_s.at[1 - c], wo_send, wo_recv, mate)
    share_wo.start()

    def project(row):
        row = _aligned(row, BLOCK)
        rows = pl.ds(row, BLOCK)
        a = xn_s[rows, :]
        block = lax.div(row, BLOCK)
        cos_in, sin_in = turn_s[0, :BLOCK, :], turn_s[1, :BLOCK, :]
        cb, sb = turn_s[0, pl.ds(BLOCK + block, 1), :], turn_s[1, pl.ds(BLOCK + block, 1), :]
        cos = cb * cos_in - sb * sin_in
        sin = sb * cos_in + cb * sin_in
        for i, to in ((0, q_s), (1, k_s)):
            t = _dot(a, w_s[i], 1, 0).astype(jnp.bfloat16)
            for h in range(heads):
                u = t[:, h * HEAD : (h + 1) * HEAD].astype(jnp.float32)
                to[h, rows, :] = (u * cos + pltpu.roll(u, HEAD // 2, 1) * sin).astype(to.dtype)
        t = _dot(a, w_s[2], 1, 0).astype(jnp.bfloat16)
        for h in range(heads):
            vt_s[h, :HEAD, rows] = t[:, h * HEAD : (h + 1) * HEAD].T

    e = HEAD**-0.5 * LOG2E

    def attend(row):
        row = _aligned(row, BLOCK)
        rows = pl.ds(row, BLOCK)
        top_s[...] = jnp.full(top_s.shape, NEG, jnp.float32)
        mix_s[...] = jnp.zeros(mix_s.shape, jnp.float32)

        def step(j, masked):
            keys = pl.ds(_aligned(j * BLOCK, BLOCK), BLOCK)
            scores = [_dot(k_s[h, keys, :], q_s[h, rows, :], 1, 1) for h in range(heads)]
            weights, keeps = [], []
            if masked:
                ok = lax.broadcasted_iota(jnp.int32, (BLOCK, BLOCK), 1) >= lax.broadcasted_iota(jnp.int32, (BLOCK, BLOCK), 0)
            for h, s in enumerate(scores):
                if masked:
                    s = jnp.where(ok, s, HIDDEN)
                old = top_s[h : h + 1, :]
                top = jnp.maximum(old, s.max(axis=0, keepdims=True))
                top_s[h : h + 1, :] = top
                weights.append(jnp.exp2((s - top) * e).astype(jnp.bfloat16))
                keeps.append(jnp.exp2((old - top) * e))
            for h, (p, keep) in enumerate(zip(weights, keeps)):
                mix_s[h] = mix_s[h] * keep + _dot(vt_s[h, :, keys], p, 1, 0)

        last = lax.div(row, BLOCK)
        lax.fori_loop(0, last, lambda j, _: step(j, False), None)
        step(last, True)
        for h in range(heads):
            out = (mix_s[h, :HEAD, :] * (1 / mix_s[h, HEAD : HEAD + 1, :])).astype(seen_s.dtype)
            seen_s[c, rows, h * HEAD : (h + 1) * HEAD] = out.T

    def seen_out(s):
        rows = pl.ds(_aligned(there + s * BLOCK + (1 - c) * HALF, HALF), HALF)
        return remote(seen_s.at[c, rows, :], seen_s.at[c, rows, :], seen_send, seen_recv.at[s], mate)

    def seen_in(s):
        rows = pl.ds(_aligned(there + s * BLOCK + c * HALF, HALF), HALF)
        return remote(seen_s.at[1 - c, rows, :], seen_s.at[1 - c, rows, :], seen_send, seen_recv.at[s], mate)

    def term_out(s):
        j = 2 * lax.rem(s, 2) + c
        src = term_s.at[pl.ds(_aligned(s * HALF, HALF), HALF), :]
        dst = got_s.at[pl.ds(_aligned(j * HALF, HALF), HALF), :]
        return remote(src, dst, row_send, term_recv.at[j], 2 * (1 - chip) + lax.div(s, 2))

    def last_out(p):
        at, rows = LAST[p]
        src = term_s.at[pl.ds(3 * HALF + at, rows), :]
        dst = got_s.at[pl.ds(_aligned((2 + c) * HALF + at, 32), rows), :]
        return remote(src, dst, row_send, term_recv.at[2 + 2 * p + c], 2 * (1 - chip) + 1)

    def term(s):
        seen_in(s).wait_recv()
        rows = pl.ds(_aligned(there + s * BLOCK + c * HALF, HALF), HALF)
        a, b = seen_s[0, rows, :], seen_s[1, rows, :]
        for n in range(0, width, 512):
            t = _dot(a, wo_s[0, :, n : n + 512], 1, 0) + _dot(b, wo_s[1, :, n : n + 512], 1, 0)
            term_s[pl.ds(_aligned(s * HALF, HALF), HALF), n : n + 512] = t.astype(term_s.dtype)

    vt_s[:, HEAD:, :] = jnp.ones((heads, PAD, 4 * own), vt_s.dtype)
    load_turn.wait()
    pltpu.make_async_copy(w_s, w_s, load_sem.at[3]).wait()
    project(mine)

    @on_core(0)
    def _():
        near_in(0).wait_recv()
        far(2, here).start()
        near_in(1).wait_recv()
        far(3, here).start()

    near_others.wait_recv()

    def local(i, _):
        at = lax.rem(2 * c + 1 + i, 4)
        project(here + at * BLOCK)
        return _

    lax.fori_loop(0, 3, local, None)
    share_wo_in.wait_recv()

    def arrived(s, _):
        @pl.when(s == 2 * c)
        def _():
            lead(there).wait_recv()
            rest(there).wait_recv()

        @pl.when(s != 2 * c)
        def _():
            far(s, there).wait_recv()

        onward(s).start()

        @pl.when(s > 0)
        def _():
            term(s - 1)
            term_out(s - 1).start()

        onward_in(s).wait_recv()
        project(there + s * BLOCK)
        attend(there + s * BLOCK)
        seen_out(s).start()
        return _

    lax.fori_loop(0, 4, arrived, None)

    def mine_out(i):
        rows = pl.ds(_aligned(mates + i * BLOCK, BLOCK), BLOCK)
        return remote(seen_s.at[c, rows, :], seen_s.at[c, rows, :], seen_send, mine_recv, mate)

    own_rows = pl.ds(_aligned(mine, BLOCK), own)
    mine_in = remote(seen_s.at[1 - c, own_rows, :], seen_s.at[1 - c, own_rows, :], seen_send, mine_recv, mate)

    def inside(i, _):
        at = lax.rem(2 * (1 - c) + i, 4)
        attend(here + at * BLOCK)

        @pl.when(i == 0)
        def _():
            term(3)
            for p in range(len(LAST)):
                last_out(p).start()

        @pl.when(i < 2)
        def _():
            mine_out(i).start()

        return _

    lax.fori_loop(0, 4, inside, None)

    def keep(i, _):
        rows = pl.ds(_aligned(mine + i * BLOCK, BLOCK), BLOCK)
        to = pl.ds(_aligned(i * BLOCK, BLOCK), BLOCK)
        a, b = seen_s[0, rows, :], seen_s[1, rows, :]
        for n in range(0, width, 512):
            t = _dot(a, wo_s[0, :, n : n + 512], 1, 0) + _dot(b, wo_s[1, :, n : n + 512], 1, 0)
            acc_s[to, n : n + 512] = t + x_s[to, n : n + 512].astype(jnp.float32)
        return _

    mine_in.wait_recv()
    lax.fori_loop(0, 2, keep, None)

    def term_in(j, at, rows, i):
        rows = pl.ds(j * HALF + at, rows)
        return remote(got_s.at[rows, :], got_s.at[rows, :], row_send, term_recv.at[i], peer)

    def finish(first, rows):
        def some(r, _):
            at = pl.ds(_aligned(first + r * 32, 32), 32)
            y_ref[at, :] = (acc_s[at, :] + got_s[at, :].astype(jnp.float32)).astype(y_ref.dtype)
            return _

        lax.fori_loop(0, rows // 32, some, None)

    for j in range(2):
        term_in(j, 0, HALF, j).wait_recv()
        finish(j * HALF, HALF)

    @on_core(0)
    def _():
        for j in range(2, 4):
            term_in(j, 0, HALF, j).wait_recv()
            finish(j * HALF, HALF)

    @on_core(1)
    def _():
        for p, (at, rows) in enumerate(LAST):
            for j in range(2, 4):
                term_in(j, at, rows, j + 2 * p).wait_recv()
                finish(j * HALF + at, rows)

    remote(xn_s, xn_s, row_send, near_recv.at[0], mate).wait_send()
    half_seen = seen_s.at[0, pl.ds(0, 2 * own), :]
    remote(half_seen, half_seen, seen_send, mine_recv, mate).wait_send()
    share_wo.wait_send()


def _tables(tokens):
    half = HEAD // 2
    rate = np.float32(THETA) ** (-np.arange(half, dtype=np.float32) / np.float32(half))
    sign = np.concatenate([-np.ones(half), np.ones(half)])

    def pair(place):
        angle = place[:, None].astype(np.float64) * np.tile(rate, 2).astype(np.float64)
        return np.cos(angle).astype(np.float32), (np.sin(angle) * sign).astype(np.float32)

    both = zip(pair(np.arange(BLOCK)), pair(np.arange(0, tokens, BLOCK)))
    return np.stack([np.concatenate(t) for t in both])


def solution(mesh):
    def step(x, gain, wq, wk, wv, wo):
        own, width = x.shape
        tokens = 4 * own
        inner = wq.shape[1]
        heads = inner // HEAD
        low = jnp.bfloat16
        dma = pltpu.SemaphoreType.DMA
        hbm = pl.BlockSpec(memory_space=pl.ANY)
        return pl.pallas_call(
            functools.partial(kernel, own),
            name="layer",
            out_shape=pltpu.VMEM((own, width), low),
            in_specs=[hbm] * 7,
            out_specs=pl.BlockSpec(memory_space=pltpu.VMEM),
            scratch_shapes=[
                pltpu.VMEM((own, width), low),
                pltpu.VMEM((width // 128, 128), low),
                pltpu.VMEM((2, BLOCK + tokens // BLOCK, HEAD), jnp.float32),
                pltpu.VMEM((tokens, width), low),
                pltpu.VMEM((3, width, inner), low),
                pltpu.VMEM((2, inner, width), low),
                pltpu.VMEM((heads, tokens, HEAD), low),
                pltpu.VMEM((heads, tokens, HEAD), low),
                pltpu.VMEM((heads, HEAD + PAD, tokens), low),
                pltpu.VMEM((2, tokens, inner), low),
                pltpu.VMEM((8, BLOCK), jnp.float32),
                pltpu.VMEM((heads, HEAD + PAD, BLOCK), jnp.float32),
                pltpu.VMEM((own, width), low),
                pltpu.VMEM((own, width), low),
                pltpu.VMEM((own, width), jnp.float32),
                dma((7,)), pltpu.SemaphoreType.REGULAR, dma, dma, dma,
                dma((3,)), dma((5,)), dma((4,)), dma((4,)), dma, dma, dma((6,)),
            ],
            compiler_params=pltpu.CompilerParams(collective_id=0, has_side_effects=True, vmem_limit_bytes=VMEM),
        )(x, gain.reshape(width // 128, 128), wq, wk, wv, wo, jnp.asarray(_tables(tokens)))

    tokens, columns = P(("dp", "tp"), None), P(None, "tp")
    return jax.shard_map(
        step,
        mesh=mesh,
        in_specs=(tokens, P(None), columns, columns, columns, P("tp", None)),
        out_specs=tokens,
        check_vma=False,
    )
```

```python
import functools

import jax
import jax.numpy as jnp
import numpy as np
from jax import lax
from jax.experimental import pallas as pl
from jax.experimental.pallas import tpu as pltpu
from jax.sharding import PartitionSpec as P

HEAD = 128
THETA = 10000
VMEM = 60 * 2**20
NEG = float(np.finfo(np.float32).min)
HIDDEN = -np.inf
LOG2E = 1.4426950408889634
MESH = pl.DeviceIdType.MESH
BLOCK = 256
HALF = BLOCK // 2
LEAD = 32
LAST = (0, 96), (96, 32)
PAD = 16


def _dot(a, b, ca, cb):
    return lax.dot_general(a, b, (((ca,), (cb,)), ((), ())), preferred_element_type=jnp.float32)


def _aligned(x, n):
    return pl.multiple_of(x, n)


def kernel(own, x_hbm, gain_hbm, wq_hbm, wk_hbm, wv_hbm, wo_hbm, turn_hbm, y_ref,
           x_s, gain_s, turn_s, xn_s, w_s, wo_s, q_s, k_s, vt_s, seen_s, top_s, mix_s, term_s, got_s, acc_s,
           load_sem, mate_sem, row_send, seen_send, wo_send, near_recv, far_recv, pass_recv, seen_recv, mine_recv, wo_recv, term_recv):
    heads = q_s.shape[0]
    width = x_s.shape[1]
    inner = heads * HEAD
    tp = lax.axis_index("tp")
    c = lax.rem(tp, 2)
    chip = lax.div(tp, 2)
    mate = tp + 1 - 2 * c
    peer = lax.rem(tp + 2, 4)
    here = chip * (2 * own)
    there = (1 - chip) * (2 * own)
    mine = here + c * own
    mates = here + (1 - c) * own

    def remote(src, dst, send, recv, device):
        return pltpu.make_async_remote_copy(src_ref=src, dst_ref=dst, send_sem=send, recv_sem=recv, device_id={"tp": device}, device_id_type=MESH)

    first = c * HALF
    order = [lax.rem(c + i, 4) for i in range(4)]

    def load_x(i, at, rows):
        rows = pl.ds(_aligned(at, LEAD), rows)
        return pltpu.make_async_copy(x_hbm.at[rows, :], x_s.at[rows, :], load_sem.at[i])

    loads_x = [load_x(0, order[0] * HALF, HALF), *(load_x(1, order[i] * HALF, HALF) for i in range(1, 4))]

    def load_w(i):
        return pltpu.make_async_copy((wq_hbm, wk_hbm, wv_hbm)[i], w_s.at[i], load_sem.at[2])

    load_wo = pltpu.make_async_copy(wo_hbm, wo_s.at[c], load_sem.at[3])
    load_gain = pltpu.make_async_copy(gain_hbm, gain_s, load_sem.at[4])
    load_turn = pltpu.make_async_copy(turn_hbm, turn_s, load_sem.at[5])

    def on_core(n):
        return pl.when(c == n)

    barrier = pltpu.get_barrier_semaphore()
    pl.semaphore_signal(barrier, inc=1, device_id={"tp": peer}, device_id_type=MESH)

    @on_core(1)
    def _():
        pl.semaphore_signal(barrier, inc=1, device_id={"tp": mate}, device_id_type=MESH)

    def near_rows(base, i, rows, at):
        rows = pl.ds(_aligned(base + i * HALF, HALF), rows)
        return remote(xn_s.at[rows, :], xn_s.at[rows, :], row_send, near_recv.at[at], mate)

    def near(i):
        return near_rows(mine, i, HALF, jnp.where(lax.rem(i, 2) == 1 - c, lax.div(i, 2), 2))

    def near_in(i):
        return near_rows(mates, 2 * i + c, HALF, i)

    near_others = near_rows(mates, 0, 2 * HALF, 2)

    def cross(base, at, rows, i):
        rows = pl.ds(_aligned(base + c * HALF + at, LEAD), rows)
        return remote(xn_s.at[rows, :], xn_s.at[rows, :], row_send, far_recv.at[i], peer)

    def far(s, base):
        return cross(base, s * BLOCK, HALF, s)

    def rest(base):
        return cross(base, 2 * c * BLOCK + LEAD, HALF - LEAD, 2 * c)

    def lead():
        to = pl.ds(_aligned(mine + first, LEAD), LEAD)
        return remote(x_hbm.at[pl.ds(_aligned(first, LEAD), LEAD), :], xn_s.at[to, :], row_send, far_recv.at[2 * c], peer)

    def onward(s):
        rows = pl.ds(_aligned(there + s * BLOCK + c * HALF, HALF), HALF)
        return remote(xn_s.at[rows, :], xn_s.at[rows, :], row_send, pass_recv.at[lax.rem(s, 2)], mate)

    def onward_in(s):
        rows = pl.ds(_aligned(there + s * BLOCK + (1 - c) * HALF, HALF), HALF)
        return remote(xn_s.at[rows, :], xn_s.at[rows, :], row_send, pass_recv.at[lax.rem(s, 2)], mate)

    def norm(rows, ref, at, to):
        def some(r, _):
            wide = ref[pl.ds(_aligned(at + r * 32, 32), 32), :].astype(jnp.float32)
            scale = lax.rsqrt(jnp.mean(wide * wide, -1, keepdims=True) + 1e-6)
            for g in range(width // 128):
                lanes = slice(g * 128, (g + 1) * 128)
                normed = wide[:, lanes] * scale * gain_s[g : g + 1, :].astype(jnp.float32)
                xn_s[pl.ds(_aligned(to + r * 32, 32), 32), lanes] = normed.astype(xn_s.dtype)
            return _

        lax.fori_loop(0, rows // 32, some, None)

    def tell_mate():
        pl.semaphore_signal(mate_sem, inc=1, device_id={"tp": mate}, device_id_type=MESH)

    @on_core(0)
    def _():
        pl.semaphore_wait(barrier, 2)
        tell_mate()

    @on_core(1)
    def _():
        pl.semaphore_wait(barrier, 1)

    lead().start()
    load_gain.start()
    for load in loads_x:
        load.start()
    for i in range(3):
        load_w(i).start()
    load_turn.start()
    load_wo.start()
    load_gain.wait()
    load_x(0, 0, HALF).wait()
    norm(HALF, x_s, first, mine + first)

    @on_core(0)
    def _():
        rest(here).start()

    @on_core(1)
    def _():
        pl.semaphore_wait(mate_sem, 1)
        tell_mate()

    near(order[0]).start()
    load_x(1, 0, 3 * HALF).wait()
    for i in range(1, 4):
        norm(HALF, x_s, order[i] * HALF, mine + order[i] * HALF)
        near(order[i]).start()
        if i == 2:

            @on_core(0)
            def _():
                far(1, here).start()

    @on_core(0)
    def _():
        pl.semaphore_wait(mate_sem, 1)

    @on_core(1)
    def _():
        near_in(0).wait_recv()
        far(0, here).start()
        near_in(1).wait_recv()
        far(1, here).start()
        rest(here).start()
        far(3, here).start()

    load_wo.wait()
    share_wo = remote(wo_s.at[c], wo_s.at[c], wo_send, wo_recv, mate)
    share_wo_in = remote(wo_s.at[1 - c], wo_s.at[1 - c], wo_send, wo_recv, mate)
    share_wo.start()

    def project(row):
        row = _aligned(row, BLOCK)
        rows = pl.ds(row, BLOCK)
        a = xn_s[rows, :]
        block = lax.div(row, BLOCK)
        cos_in, sin_in = turn_s[0, :BLOCK, :], turn_s[1, :BLOCK, :]
        cb, sb = turn_s[0, pl.ds(BLOCK + block, 1), :], turn_s[1, pl.ds(BLOCK + block, 1), :]
        cos = cb * cos_in - sb * sin_in
        sin = sb * cos_in + cb * sin_in
        for i, to in ((0, q_s), (1, k_s)):
            t = _dot(a, w_s[i], 1, 0).astype(jnp.bfloat16)
            for h in range(heads):
                u = t[:, h * HEAD : (h + 1) * HEAD].astype(jnp.float32)
                to[h, rows, :] = (u * cos + pltpu.roll(u, HEAD // 2, 1) * sin).astype(to.dtype)
        t = _dot(a, w_s[2], 1, 0).astype(jnp.bfloat16)
        for h in range(heads):
            vt_s[h, :HEAD, rows] = t[:, h * HEAD : (h + 1) * HEAD].T

    e = HEAD**-0.5 * LOG2E

    def attend(row):
        row = _aligned(row, BLOCK)
        rows = pl.ds(row, BLOCK)
        top_s[...] = jnp.full(top_s.shape, NEG, jnp.float32)
        mix_s[...] = jnp.zeros(mix_s.shape, jnp.float32)

        def step(j, masked):
            keys = pl.ds(_aligned(j * BLOCK, BLOCK), BLOCK)
            scores = [_dot(k_s[h, keys, :], q_s[h, rows, :], 1, 1) for h in range(heads)]
            weights, keeps = [], []
            if masked:
                ok = lax.broadcasted_iota(jnp.int32, (BLOCK, BLOCK), 1) >= lax.broadcasted_iota(jnp.int32, (BLOCK, BLOCK), 0)
            for h, s in enumerate(scores):
                if masked:
                    s = jnp.where(ok, s, HIDDEN)
                old = top_s[h : h + 1, :]
                top = jnp.maximum(old, s.max(axis=0, keepdims=True))
                top_s[h : h + 1, :] = top
                weights.append(jnp.exp2((s - top) * e).astype(jnp.bfloat16))
                keeps.append(jnp.exp2((old - top) * e))
            for h, (p, keep) in enumerate(zip(weights, keeps)):
                mix_s[h] = mix_s[h] * keep + _dot(vt_s[h, :, keys], p, 1, 0)

        last = lax.div(row, BLOCK)
        lax.fori_loop(0, last, lambda j, _: step(j, False), None)
        step(last, True)
        for h in range(heads):
            out = (mix_s[h, :HEAD, :] * (1 / mix_s[h, HEAD : HEAD + 1, :])).astype(seen_s.dtype)
            seen_s[c, rows, h * HEAD : (h + 1) * HEAD] = out.T

    def seen_out(s):
        rows = pl.ds(_aligned(there + s * BLOCK + (1 - c) * HALF, HALF), HALF)
        return remote(seen_s.at[c, rows, :], seen_s.at[c, rows, :], seen_send, seen_recv.at[lax.rem(s, 2)], mate)

    def seen_in(s):
        rows = pl.ds(_aligned(there + s * BLOCK + c * HALF, HALF), HALF)
        return remote(seen_s.at[1 - c, rows, :], seen_s.at[1 - c, rows, :], seen_send, seen_recv.at[lax.rem(s, 2)], mate)

    def term_out(block, at, rows, to, i):
        src = term_s.at[pl.ds(block * HALF + at, rows), :]
        dst = got_s.at[pl.ds(_aligned((2 * c + block % 2) * HALF + at, 32), rows), :]
        return remote(src, dst, row_send, term_recv.at[i], 2 * (1 - chip) + to)

    def term(s):
        seen_in(s).wait_recv()
        rows = pl.ds(_aligned(there + s * BLOCK + c * HALF, HALF), HALF)
        a, b = seen_s[0, rows, :], seen_s[1, rows, :]
        for n in range(0, width, 512):
            t = _dot(a, wo_s[0, :, n : n + 512], 1, 0) + _dot(b, wo_s[1, :, n : n + 512], 1, 0)
            term_s[pl.ds(_aligned(s * HALF, HALF), HALF), n : n + 512] = t.astype(term_s.dtype)

    vt_s[:, HEAD:, :] = jnp.ones((heads, PAD, 4 * own), vt_s.dtype)
    load_turn.wait()
    pltpu.make_async_copy(w_s, w_s, load_sem.at[2]).wait()
    project(mine)

    @on_core(0)
    def _():
        near_in(0).wait_recv()
        far(2, here).start()
        near_in(1).wait_recv()
        far(3, here).start()

    near_others.wait_recv()

    def local(i, _):
        at = lax.rem(2 * c + 1 + i, 4)
        project(here + at * BLOCK)
        return _

    lax.fori_loop(0, 3, local, None)
    share_wo_in.wait_recv()

    def arrived(s, _):
        far(s, there).wait_recv()

        @pl.when(s == 2 * c)
        def _():
            at = there + c * own + first
            norm(LEAD, xn_s, at, at)

        onward(s).start()

        @pl.when(s > 0)
        def _():
            term(s - 1)

        @pl.when(s == 2)
        def _():
            term_out(0, 0, 2 * HALF, 0, 0).start()

        @pl.when(s == 3)
        def _():
            term_out(2, 0, HALF, 1, 0).start()

        onward_in(s).wait_recv()
        project(there + s * BLOCK)
        attend(there + s * BLOCK)
        seen_out(s).start()
        return _

    lax.fori_loop(0, 4, arrived, None)

    def mine_out(i):
        rows = pl.ds(_aligned(mates + i * BLOCK, BLOCK), BLOCK)
        return remote(seen_s.at[c, rows, :], seen_s.at[c, rows, :], seen_send, mine_recv, mate)

    own_rows = pl.ds(_aligned(mine, BLOCK), own)
    mine_in = remote(seen_s.at[1 - c, own_rows, :], seen_s.at[1 - c, own_rows, :], seen_send, mine_recv, mate)

    def inside(i, _):
        at = lax.rem(2 * (1 - c) + i, 4)
        attend(here + at * BLOCK)

        @pl.when(i == 0)
        def _():
            term(3)
            for i, (first_row, rows) in enumerate(LAST):
                term_out(3, first_row, rows, 1, 1 + i).start()

        @pl.when(i < 2)
        def _():
            mine_out(i).start()

        return _

    lax.fori_loop(0, 4, inside, None)

    def keep(i, _):
        rows = pl.ds(_aligned(mine + i * BLOCK, BLOCK), BLOCK)
        to = pl.ds(_aligned(i * BLOCK, BLOCK), BLOCK)
        a, b = seen_s[0, rows, :], seen_s[1, rows, :]
        for n in range(0, width, 512):
            t = _dot(a, wo_s[0, :, n : n + 512], 1, 0) + _dot(b, wo_s[1, :, n : n + 512], 1, 0)
            acc_s[to, n : n + 512] = t + x_s[to, n : n + 512].astype(jnp.float32)
        return _

    mine_in.wait_recv()
    lax.fori_loop(0, 2, keep, None)

    def terms_in(rows, i):
        rows = pl.ds(0, 2 * rows)
        remote(got_s.at[rows, :], got_s.at[rows, :], row_send, term_recv.at[i], peer).wait_recv()

    def finish(block, first, rows):
        for j in range(2):

            def some(r, _):
                at = pl.ds(_aligned((2 * block + j) * HALF + first + r * 32, 32), 32)
                got = pl.ds(_aligned((2 * j + block) * HALF + first + r * 32, 32), 32)
                y_ref[at, :] = (acc_s[at, :] + got_s[got, :].astype(jnp.float32)).astype(y_ref.dtype)
                return _

            lax.fori_loop(0, rows // 32, some, None)

    @on_core(0)
    def _():
        terms_in(2 * HALF, 0)
        finish(0, 0, HALF)
        finish(1, 0, HALF)

    @on_core(1)
    def _():
        terms_in(HALF, 0)
        finish(0, 0, HALF)
        for i, (first_row, rows) in enumerate(LAST):
            terms_in(rows, 1 + i)
            finish(1, first_row, rows)

    remote(xn_s, xn_s, row_send, near_recv.at[0], mate).wait_send()
    half_seen = seen_s.at[0, pl.ds(0, 2 * own), :]
    remote(half_seen, half_seen, seen_send, mine_recv, mate).wait_send()
    share_wo.wait_send()


def _tables(tokens):
    half = HEAD // 2
    rate = np.float32(THETA) ** (-np.arange(half, dtype=np.float32) / np.float32(half))
    sign = np.concatenate([-np.ones(half), np.ones(half)])

    def pair(place):
        angle = place[:, None].astype(np.float64) * np.tile(rate, 2).astype(np.float64)
        return np.cos(angle).astype(np.float32), (np.sin(angle) * sign).astype(np.float32)

    both = zip(pair(np.arange(BLOCK)), pair(np.arange(0, tokens, BLOCK)))
    return np.stack([np.concatenate(t) for t in both])


def solution(mesh):
    def step(x, gain, wq, wk, wv, wo):
        own, width = x.shape
        tokens = 4 * own
        inner = wq.shape[1]
        heads = inner // HEAD
        low = jnp.bfloat16
        dma = pltpu.SemaphoreType.DMA
        hbm = pl.BlockSpec(memory_space=pl.ANY)
        return pl.pallas_call(
            functools.partial(kernel, own),
            name="layer",
            out_shape=pltpu.VMEM((own, width), low),
            in_specs=[hbm] * 7,
            out_specs=pl.BlockSpec(memory_space=pltpu.VMEM),
            scratch_shapes=[
                pltpu.VMEM((own, width), low),
                pltpu.VMEM((width // 128, 128), low),
                pltpu.VMEM((2, BLOCK + tokens // BLOCK, HEAD), jnp.float32),
                pltpu.VMEM((tokens, width), low),
                pltpu.VMEM((3, width, inner), low),
                pltpu.VMEM((2, inner, width), low),
                pltpu.VMEM((heads, tokens, HEAD), low),
                pltpu.VMEM((heads, tokens, HEAD), low),
                pltpu.VMEM((heads, HEAD + PAD, tokens), low),
                pltpu.VMEM((2, tokens, inner), low),
                pltpu.VMEM((8, BLOCK), jnp.float32),
                pltpu.VMEM((heads, HEAD + PAD, BLOCK), jnp.float32),
                pltpu.VMEM((own, width), low),
                pltpu.VMEM((own, width), low),
                pltpu.VMEM((own, width), jnp.float32),
                dma((6,)), pltpu.SemaphoreType.REGULAR, dma, dma, dma,
                dma((3,)), dma((4,)), dma((2,)), dma((2,)), dma, dma, dma((3,)),
            ],
            compiler_params=pltpu.CompilerParams(collective_id=0, has_side_effects=True, vmem_limit_bytes=VMEM),
        )(x, gain.reshape(width // 128, 128), wq, wk, wv, wo, jnp.asarray(_tables(tokens)))

    tokens, columns = P(("dp", "tp"), None), P(None, "tp")
    return jax.shard_map(
        step,
        mesh=mesh,
        in_specs=(tokens, P(None), columns, columns, columns, P("tp", None)),
        out_specs=tokens,
        check_vma=False,
    )
```

```python
import functools

import jax
import jax.numpy as jnp
import numpy as np
from jax import lax
from jax.experimental import pallas as pl
from jax.experimental.pallas import tpu as pltpu
from jax.sharding import PartitionSpec as P

HEAD = 128
THETA = 10000
VMEM = 60 * 2**20
NEG = float(np.finfo(np.float32).min)
HIDDEN = -np.inf
LOG2E = 1.4426950408889634
MESH = pl.DeviceIdType.MESH
BLOCK = 256
HALF = BLOCK // 2
LEAD = 32
LAST = (0, 112), (112, 16)
PAD = 16


def _dot(a, b, ca, cb):
    return lax.dot_general(a, b, (((ca,), (cb,)), ((), ())), preferred_element_type=jnp.float32)


def _aligned(x, n):
    return pl.multiple_of(x, n)


def kernel(own, x_hbm, gain_hbm, wq_hbm, wk_hbm, wv_hbm, wo_hbm, turn_hbm, y_ref,
           x_s, gain_s, turn_s, xn_s, w_s, wo_s, q_s, k_s, vt_s, seen_s, top_s, mix_s, term_s, got_s, acc_s,
           load_sem, mate_sem, row_send, seen_send, near_recv, far_recv, pass_recv, seen_recv, mine_recv, wo_recv, term_recv):
    heads = q_s.shape[0]
    width = x_s.shape[1]
    inner = heads * HEAD
    tp = lax.axis_index("tp")
    c = lax.rem(tp, 2)
    chip = lax.div(tp, 2)
    mate = tp + 1 - 2 * c
    peer = lax.rem(tp + 2, 4)
    here = chip * (2 * own)
    there = (1 - chip) * (2 * own)
    mine = here + c * own
    mates = here + (1 - c) * own

    def remote(src, dst, send, recv, device):
        return pltpu.make_async_remote_copy(src_ref=src, dst_ref=dst, send_sem=send, recv_sem=recv, device_id={"tp": device}, device_id_type=MESH)

    first = c * HALF
    order = [lax.rem(c + i, 4) for i in range(4)]

    def load_x(i, at, rows):
        rows = pl.ds(_aligned(at, LEAD), rows)
        return pltpu.make_async_copy(x_hbm.at[rows, :], x_s.at[rows, :], load_sem.at[i])

    loads_x = [load_x(1, order[0] * HALF, HALF), *(load_x(2, order[i] * HALF, HALF) for i in range(1, 4))]

    def load_w(i):
        return pltpu.make_async_copy((wq_hbm, wk_hbm, wv_hbm)[i], w_s.at[i], load_sem.at[1])

    load_wo = pltpu.make_async_copy(wo_hbm, wo_s.at[c], load_sem.at[2])
    load_gain = pltpu.make_async_copy(gain_hbm, gain_s, load_sem.at[0])
    load_turn = pltpu.make_async_copy(turn_hbm, turn_s, load_sem.at[0])

    def on_core(n):
        return pl.when(c == n)

    barrier = pltpu.get_barrier_semaphore()
    pl.semaphore_signal(barrier, inc=1, device_id={"tp": peer}, device_id_type=MESH)

    @on_core(1)
    def _():
        pl.semaphore_signal(barrier, inc=1, device_id={"tp": mate}, device_id_type=MESH)

    def near_rows(base, i, rows):
        rows = pl.ds(_aligned(base + i * HALF, HALF), rows)
        return remote(xn_s.at[rows, :], xn_s.at[rows, :], row_send, near_recv, mate)

    def near(i):
        return near_rows(mine, i, HALF)

    near_in = near_rows(mates, 0, own)

    def cross(base, at, rows, i):
        rows = pl.ds(_aligned(base + c * HALF + at, LEAD), rows)
        return remote(xn_s.at[rows, :], xn_s.at[rows, :], row_send, far_recv.at[i], peer)

    def far(s, base):
        return cross(base, s * BLOCK, HALF, s)

    def rest(base):
        return cross(base, 2 * c * BLOCK + LEAD, HALF - LEAD, 2 * c)

    def lead():
        to = pl.ds(_aligned(mine + first, LEAD), LEAD)
        return remote(x_hbm.at[pl.ds(_aligned(first, LEAD), LEAD), :], xn_s.at[to, :], row_send, far_recv.at[2 * c], peer)

    def onward(s):
        rows = pl.ds(_aligned(there + s * BLOCK + c * HALF, HALF), HALF)
        return remote(xn_s.at[rows, :], xn_s.at[rows, :], row_send, pass_recv, mate)

    def onward_in(s):
        rows = pl.ds(_aligned(there + s * BLOCK + (1 - c) * HALF, HALF), HALF)
        return remote(xn_s.at[rows, :], xn_s.at[rows, :], row_send, pass_recv, mate)

    def norm(rows, ref, at, to):
        def some(r, _):
            wide = ref[pl.ds(_aligned(at + r * 32, 32), 32), :].astype(jnp.float32)
            scale = lax.rsqrt(jnp.mean(wide * wide, -1, keepdims=True) + 1e-6)
            for g in range(width // 128):
                lanes = slice(g * 128, (g + 1) * 128)
                normed = wide[:, lanes] * scale * gain_s[g : g + 1, :].astype(jnp.float32)
                xn_s[pl.ds(_aligned(to + r * 32, 32), 32), lanes] = normed.astype(xn_s.dtype)
            return _

        lax.fori_loop(0, rows // 32, some, None)

    def tell_mate():
        pl.semaphore_signal(mate_sem, inc=1, device_id={"tp": mate}, device_id_type=MESH)

    @on_core(0)
    def _():
        pl.semaphore_wait(barrier, 2)
        tell_mate()

    @on_core(1)
    def _():
        pl.semaphore_wait(barrier, 1)

    lead().start()
    load_gain.start()
    for load in loads_x:
        load.start()
    load_gain.wait()
    load_turn.start()
    load_x(1, 0, HALF).wait()
    for i in range(3):
        load_w(i).start()
    norm(HALF, x_s, first, mine + first)

    @on_core(0)
    def _():
        rest(here).start()

    @on_core(1)
    def _():
        pl.semaphore_wait(mate_sem, 1)
        tell_mate()

    near(order[0]).start()
    load_x(2, 0, 3 * HALF).wait()
    load_wo.start()
    for i in range(1, 4):
        norm(HALF, x_s, order[i] * HALF, mine + order[i] * HALF)
        near(order[i]).start()
        if i == 2:

            @on_core(0)
            def _():
                far(1, here).start()

    @on_core(0)
    def _():
        pl.semaphore_wait(mate_sem, 1)

    @on_core(1)
    def _():
        near_in.wait_recv()
        far(0, here).start()
        far(1, here).start()
        rest(here).start()
        far(3, here).start()

    load_wo.wait()
    share_wo = remote(wo_s.at[c], wo_s.at[c], seen_send, wo_recv, mate)
    share_wo_in = remote(wo_s.at[1 - c], wo_s.at[1 - c], seen_send, wo_recv, mate)
    share_wo.start()

    def project(row):
        row = _aligned(row, BLOCK)
        rows = pl.ds(row, BLOCK)
        a = xn_s[rows, :]
        block = lax.div(row, BLOCK)
        cos_in, sin_in = turn_s[0, :BLOCK, :], turn_s[1, :BLOCK, :]
        cb, sb = turn_s[0, pl.ds(BLOCK + block, 1), :], turn_s[1, pl.ds(BLOCK + block, 1), :]
        cos = cb * cos_in - sb * sin_in
        sin = sb * cos_in + cb * sin_in
        for i, to in ((0, q_s), (1, k_s)):
            t = _dot(a, w_s[i], 1, 0).astype(jnp.bfloat16)
            for h in range(heads):
                u = t[:, h * HEAD : (h + 1) * HEAD].astype(jnp.float32)
                to[h, rows, :] = (u * cos + pltpu.roll(u, HEAD // 2, 1) * sin).astype(to.dtype)
        t = _dot(a, w_s[2], 1, 0).astype(jnp.bfloat16)
        for h in range(heads):
            vt_s[h, :HEAD, rows] = t[:, h * HEAD : (h + 1) * HEAD].T

    e = HEAD**-0.5 * LOG2E

    def attend(row):
        row = _aligned(row, BLOCK)
        rows = pl.ds(row, BLOCK)
        top_s[...] = jnp.full(top_s.shape, NEG, jnp.float32)
        mix_s[...] = jnp.zeros(mix_s.shape, jnp.float32)

        def step(j, masked):
            keys = pl.ds(_aligned(j * BLOCK, BLOCK), BLOCK)
            scores = [_dot(k_s[h, keys, :], q_s[h, rows, :], 1, 1) for h in range(heads)]
            weights, keeps = [], []
            if masked:
                ok = lax.broadcasted_iota(jnp.int32, (BLOCK, BLOCK), 1) >= lax.broadcasted_iota(jnp.int32, (BLOCK, BLOCK), 0)
            for h, s in enumerate(scores):
                if masked:
                    s = jnp.where(ok, s, HIDDEN)
                old = top_s[h : h + 1, :]
                top = jnp.maximum(old, s.max(axis=0, keepdims=True))
                top_s[h : h + 1, :] = top
                weights.append(jnp.exp2((s - top) * e).astype(jnp.bfloat16))
                keeps.append(jnp.exp2((old - top) * e))
            for h, (p, keep) in enumerate(zip(weights, keeps)):
                mix_s[h] = mix_s[h] * keep + _dot(vt_s[h, :, keys], p, 1, 0)

        last = lax.div(row, BLOCK)
        lax.fori_loop(0, last, lambda j, _: step(j, False), None)
        step(last, True)
        for h in range(heads):
            out = (mix_s[h, :HEAD, :] * (1 / mix_s[h, HEAD : HEAD + 1, :])).astype(seen_s.dtype)
            seen_s[c, rows, h * HEAD : (h + 1) * HEAD] = out.T

    def seen_out(s):
        rows = pl.ds(_aligned(there + s * BLOCK + (1 - c) * HALF, HALF), HALF)
        return remote(seen_s.at[c, rows, :], seen_s.at[c, rows, :], seen_send, seen_recv, mate)

    def seen_in(s):
        rows = pl.ds(_aligned(there + s * BLOCK + c * HALF, HALF), HALF)
        return remote(seen_s.at[1 - c, rows, :], seen_s.at[1 - c, rows, :], seen_send, seen_recv, mate)

    def term_out(block, at, rows, to, i):
        src = term_s.at[pl.ds(block * HALF + at, rows), :]
        dst = got_s.at[pl.ds(_aligned((2 * c + block % 2) * HALF + at, 16), rows), :]
        return remote(src, dst, row_send, term_recv.at[i], 2 * (1 - chip) + to)

    def term(s):
        seen_in(s).wait_recv()
        rows = pl.ds(_aligned(there + s * BLOCK + c * HALF, HALF), HALF)
        a, b = seen_s[0, rows, :], seen_s[1, rows, :]
        for n in range(0, width, 512):
            t = _dot(a, wo_s[0, :, n : n + 512], 1, 0) + _dot(b, wo_s[1, :, n : n + 512], 1, 0)
            term_s[pl.ds(_aligned(s * HALF, HALF), HALF), n : n + 512] = t.astype(term_s.dtype)

    vt_s[:, HEAD:, :] = jnp.ones((heads, PAD, 4 * own), vt_s.dtype)
    load_turn.wait()
    pltpu.make_async_copy(w_s, w_s, load_sem.at[1]).wait()
    project(mine)

    @on_core(0)
    def _():
        near_in.wait_recv()
        far(2, here).start()
        far(3, here).start()


    def local(i, _):
        at = lax.rem(2 * c + 1 + i, 4)
        project(here + at * BLOCK)
        return _

    lax.fori_loop(0, 3, local, None)
    share_wo_in.wait_recv()
    share_wo.wait_send()

    def arrived(s, _):
        far(s, there).wait_recv()

        @pl.when(s == 2 * c)
        def _():
            at = there + c * own + first
            norm(LEAD, xn_s, at, at)

        @pl.when(s > 0)
        def _():
            term(s - 1)

        @pl.when(s == 2)
        def _():
            term_out(0, 0, 2 * HALF, 0, 0).start()

        @pl.when(s == 3)
        def _():
            term_out(2, 0, HALF, 1, 0).start()

        onward(s).start()
        onward_in(s).wait_recv()
        project(there + s * BLOCK)
        attend(there + s * BLOCK)
        seen_out(s).start()
        return _

    lax.fori_loop(0, 4, arrived, None)

    def mine_out(i):
        rows = pl.ds(_aligned(mates + i * BLOCK, BLOCK), BLOCK)
        return remote(seen_s.at[c, rows, :], seen_s.at[c, rows, :], seen_send, mine_recv, mate)

    own_rows = pl.ds(_aligned(mine, BLOCK), own)
    mine_in = remote(seen_s.at[1 - c, own_rows, :], seen_s.at[1 - c, own_rows, :], seen_send, mine_recv, mate)

    def inside(i, _):
        at = lax.rem(2 * (1 - c) + i, 4)
        attend(here + at * BLOCK)

        @pl.when(i == 0)
        def _():
            term(3)
            for i, (first_row, rows) in enumerate(LAST):
                term_out(3, first_row, rows, 1, 1 + i).start()

        @pl.when(i < 2)
        def _():
            mine_out(i).start()

        return _

    lax.fori_loop(0, 4, inside, None)

    def keep(i, _):
        rows = pl.ds(_aligned(mine + i * BLOCK, BLOCK), BLOCK)
        to = pl.ds(_aligned(i * BLOCK, BLOCK), BLOCK)
        a, b = seen_s[0, rows, :], seen_s[1, rows, :]
        for n in range(0, width, 512):
            t = _dot(a, wo_s[0, :, n : n + 512], 1, 0) + _dot(b, wo_s[1, :, n : n + 512], 1, 0)
            acc_s[to, n : n + 512] = t + x_s[to, n : n + 512].astype(jnp.float32)
        return _

    mine_in.wait_recv()
    lax.fori_loop(0, 2, keep, None)

    def terms_in(rows, i):
        rows = pl.ds(0, 2 * rows)
        remote(got_s.at[rows, :], got_s.at[rows, :], row_send, term_recv.at[i], peer).wait_recv()

    def finish(block, first, rows):
        for j in range(2):

            def some(r, _):
                at = pl.ds(_aligned((2 * block + j) * HALF + first + r * 16, 16), 16)
                got = pl.ds(_aligned((2 * j + block) * HALF + first + r * 16, 16), 16)
                y_ref[at, :] = (acc_s[at, :] + got_s[got, :].astype(jnp.float32)).astype(y_ref.dtype)
                return _

            lax.fori_loop(0, rows // 16, some, None)

    @on_core(0)
    def _():
        terms_in(2 * HALF, 0)
        finish(0, 0, HALF)
        finish(1, 0, HALF)

    @on_core(1)
    def _():
        terms_in(HALF, 0)
        finish(0, 0, HALF)
        for i, (first_row, rows) in enumerate(LAST):
            terms_in(rows, 1 + i)
            finish(1, first_row, rows)

    remote(xn_s, xn_s, row_send, near_recv, mate).wait_send()
    half_seen = seen_s.at[0, pl.ds(0, 2 * own), :]
    remote(half_seen, half_seen, seen_send, mine_recv, mate).wait_send()


def _tables(tokens):
    half = HEAD // 2
    rate = np.float32(THETA) ** (-np.arange(half, dtype=np.float32) / np.float32(half))
    sign = np.concatenate([-np.ones(half), np.ones(half)])

    def pair(place):
        angle = place[:, None].astype(np.float64) * np.tile(rate, 2).astype(np.float64)
        return np.cos(angle).astype(np.float32), (np.sin(angle) * sign).astype(np.float32)

    both = zip(pair(np.arange(BLOCK)), pair(np.arange(0, tokens, BLOCK)))
    return np.stack([np.concatenate(t) for t in both])


def solution(mesh):
    def step(x, gain, wq, wk, wv, wo):
        own, width = x.shape
        tokens = 4 * own
        inner = wq.shape[1]
        heads = inner // HEAD
        low = jnp.bfloat16
        dma = pltpu.SemaphoreType.DMA
        hbm = pl.BlockSpec(memory_space=pl.ANY)
        return pl.pallas_call(
            functools.partial(kernel, own),
            name="layer",
            out_shape=pltpu.VMEM((own, width), low),
            in_specs=[hbm] * 7,
            out_specs=pl.BlockSpec(memory_space=pltpu.VMEM),
            scratch_shapes=[
                pltpu.VMEM((own, width), low),
                pltpu.VMEM((width // 128, 128), low),
                pltpu.VMEM((2, BLOCK + tokens // BLOCK, HEAD), jnp.float32),
                pltpu.VMEM((tokens, width), low),
                pltpu.VMEM((3, width, inner), low),
                pltpu.VMEM((2, inner, width), low),
                pltpu.VMEM((heads, tokens, HEAD), low),
                pltpu.VMEM((heads, tokens, HEAD), low),
                pltpu.VMEM((heads, HEAD + PAD, tokens), low),
                pltpu.VMEM((2, tokens, inner), low),
                pltpu.VMEM((8, BLOCK), jnp.float32),
                pltpu.VMEM((heads, HEAD + PAD, BLOCK), jnp.float32),
                pltpu.VMEM((own, width), low),
                pltpu.VMEM((own, width), low),
                pltpu.VMEM((own, width), jnp.float32),
                dma((3,)), pltpu.SemaphoreType.REGULAR, dma, dma,
                dma, dma((4,)), dma, dma, dma, dma, dma((3,)),
            ],
            compiler_params=pltpu.CompilerParams(collective_id=0, has_side_effects=True, vmem_limit_bytes=VMEM),
        )(x, gain.reshape(width // 128, 128), wq, wk, wv, wo, jnp.asarray(_tables(tokens)))

    tokens, columns = P(("dp", "tp"), None), P(None, "tp")
    return jax.shard_map(
        step,
        mesh=mesh,
        in_specs=(tokens, P(None), columns, columns, columns, P("tp", None)),
        out_specs=tokens,
        check_vma=False,
    )
```

```python
import functools

import jax
import jax.numpy as jnp
import numpy as np
from jax import lax
from jax.experimental import pallas as pl
from jax.experimental.pallas import tpu as pltpu
from jax.sharding import PartitionSpec as P

HEAD = 128
THETA = 10000
VMEM = 60 * 2**20
NEG = float(np.finfo(np.float32).min)
HIDDEN = -np.inf
LOG2E = 1.4426950408889634
MESH = pl.DeviceIdType.MESH
BLOCK = 256
HALF = BLOCK // 2
LEAD = 32
LAST = (0, 112), (112, 16)
PAD = 16


def _dot(a, b, ca, cb):
    return lax.dot_general(a, b, (((ca,), (cb,)), ((), ())), preferred_element_type=jnp.float32)


def _aligned(x, n):
    return pl.multiple_of(x, n)


def kernel(own, x_hbm, gain_hbm, wq_hbm, wk_hbm, wv_hbm, wo_hbm, turn_hbm, y_ref,
           x_s, gain_s, turn_s, xn_s, w_s, wo_s, q_s, k_s, vt_s, seen_s, top_s, mix_s, term_s, got_s, acc_s,
           load_sem, mate_sem, row_send, seen_send, near_recv, far_recv, pass_recv, seen_recv, wo_recv, term_recv):
    heads = q_s.shape[0]
    width = x_s.shape[1]
    inner = heads * HEAD
    tp = lax.axis_index("tp")
    c = lax.rem(tp, 2)
    chip = lax.div(tp, 2)
    mate = tp + 1 - 2 * c
    peer = lax.rem(tp + 2, 4)
    here = chip * (2 * own)
    there = (1 - chip) * (2 * own)
    mine = here + c * own
    mates = here + (1 - c) * own

    def remote(src, dst, send, recv, device):
        return pltpu.make_async_remote_copy(src_ref=src, dst_ref=dst, send_sem=send, recv_sem=recv, device_id={"tp": device}, device_id_type=MESH)

    first = c * HALF
    order = [lax.rem(c + i, 4) for i in range(4)]

    def load_x(i, at, rows):
        rows = pl.ds(_aligned(at, LEAD), rows)
        return pltpu.make_async_copy(x_hbm.at[rows, :], x_s.at[rows, :], load_sem.at[i])

    loads_x = [load_x(1, order[0] * HALF, HALF), *(load_x(0, order[i] * HALF, HALF) for i in range(1, 4))]

    def load_w(i):
        return pltpu.make_async_copy((wq_hbm, wk_hbm, wv_hbm)[i], w_s.at[i], load_sem.at[1])

    load_wo = pltpu.make_async_copy(wo_hbm, wo_s.at[c], load_sem.at[0])
    load_gain = pltpu.make_async_copy(gain_hbm, gain_s, load_sem.at[0])
    load_turn = pltpu.make_async_copy(turn_hbm, turn_s, load_sem.at[0])

    def on_core(n):
        return pl.when(c == n)

    barrier = pltpu.get_barrier_semaphore()
    pl.semaphore_signal(barrier, inc=1, device_id={"tp": peer}, device_id_type=MESH)

    @on_core(1)
    def _():
        pl.semaphore_signal(barrier, inc=1, device_id={"tp": mate}, device_id_type=MESH)

    def near_rows(base, i, rows):
        rows = pl.ds(_aligned(base + i * HALF, HALF), rows)
        return remote(xn_s.at[rows, :], xn_s.at[rows, :], row_send, near_recv, mate)

    def near(i):
        return near_rows(mine, i, HALF)

    near_in = near_rows(mates, 0, own)

    def cross(base, at, rows, i):
        rows = pl.ds(_aligned(base + c * HALF + at, LEAD), rows)
        return remote(xn_s.at[rows, :], xn_s.at[rows, :], row_send, far_recv.at[i], peer)

    def far(s, base):
        return cross(base, s * BLOCK, HALF, s)

    def rest(base):
        return cross(base, 2 * c * BLOCK + LEAD, HALF - LEAD, 2 * c)

    def lead():
        to = pl.ds(_aligned(mine + first, LEAD), LEAD)
        return remote(x_hbm.at[pl.ds(_aligned(first, LEAD), LEAD), :], xn_s.at[to, :], row_send, far_recv.at[2 * c], peer)

    def onward(s):
        rows = pl.ds(_aligned(there + s * BLOCK + c * HALF, HALF), HALF)
        return remote(xn_s.at[rows, :], xn_s.at[rows, :], row_send, pass_recv, mate)

    def onward_in(s):
        rows = pl.ds(_aligned(there + s * BLOCK + (1 - c) * HALF, HALF), HALF)
        return remote(xn_s.at[rows, :], xn_s.at[rows, :], row_send, pass_recv, mate)

    def norm(rows, ref, at, to):
        def some(r, _):
            wide = ref[pl.ds(_aligned(at + r * 32, 32), 32), :].astype(jnp.float32)
            scale = lax.rsqrt(jnp.mean(wide * wide, -1, keepdims=True) + 1e-6)
            for g in range(width // 128):
                lanes = slice(g * 128, (g + 1) * 128)
                normed = wide[:, lanes] * scale * gain_s[g : g + 1, :].astype(jnp.float32)
                xn_s[pl.ds(_aligned(to + r * 32, 32), 32), lanes] = normed.astype(xn_s.dtype)
            return _

        lax.fori_loop(0, rows // 32, some, None)

    def tell_mate():
        pl.semaphore_signal(mate_sem, inc=1, device_id={"tp": mate}, device_id_type=MESH)

    @on_core(0)
    def _():
        pl.semaphore_wait(barrier, 2)
        tell_mate()

    @on_core(1)
    def _():
        pl.semaphore_wait(barrier, 1)

    lead().start()
    load_gain.start()
    loads_x[0].start()
    load_gain.wait()
    for load in loads_x[1:]:
        load.start()
    load_x(1, 0, HALF).wait()
    for i in range(3):
        load_w(i).start()
    norm(HALF, x_s, first, mine + first)

    @on_core(0)
    def _():
        rest(here).start()

    @on_core(1)
    def _():
        pl.semaphore_wait(mate_sem, 1)
        tell_mate()

    near(order[0]).start()
    load_x(0, 0, 3 * HALF).wait()
    load_wo.start()
    for i in range(1, 4):
        norm(HALF, x_s, order[i] * HALF, mine + order[i] * HALF)
        near(order[i]).start()
        if i == 2:

            @on_core(0)
            def _():
                far(1, here).start()

    @on_core(0)
    def _():
        pl.semaphore_wait(mate_sem, 1)

    @on_core(1)
    def _():
        near_in.wait_recv()
        far(0, here).start()
        far(1, here).start()
        rest(here).start()
        far(3, here).start()

    load_wo.wait()
    load_turn.start()
    share_wo = remote(wo_s.at[c], wo_s.at[c], seen_send, wo_recv, mate)
    share_wo_in = remote(wo_s.at[1 - c], wo_s.at[1 - c], seen_send, wo_recv, mate)
    share_wo.start()

    def project(row):
        row = _aligned(row, BLOCK)
        rows = pl.ds(row, BLOCK)
        a = xn_s[rows, :]
        block = lax.div(row, BLOCK)
        cos_in, sin_in = turn_s[0, :BLOCK, :], turn_s[1, :BLOCK, :]
        cb, sb = turn_s[0, pl.ds(BLOCK + block, 1), :], turn_s[1, pl.ds(BLOCK + block, 1), :]
        cos = cb * cos_in - sb * sin_in
        sin = sb * cos_in + cb * sin_in
        for i, to in ((0, q_s), (1, k_s)):
            t = _dot(a, w_s[i], 1, 0).astype(jnp.bfloat16)
            for h in range(heads):
                u = t[:, h * HEAD : (h + 1) * HEAD].astype(jnp.float32)
                to[h, rows, :] = (u * cos + pltpu.roll(u, HEAD // 2, 1) * sin).astype(to.dtype)
        t = _dot(a, w_s[2], 1, 0).astype(jnp.bfloat16)
        for h in range(heads):
            vt_s[h, :HEAD, rows] = t[:, h * HEAD : (h + 1) * HEAD].T

    e = HEAD**-0.5 * LOG2E

    def attend(row):
        row = _aligned(row, BLOCK)
        rows = pl.ds(row, BLOCK)
        top_s[...] = jnp.full(top_s.shape, NEG, jnp.float32)
        mix_s[...] = jnp.zeros(mix_s.shape, jnp.float32)

        def step(j, masked):
            keys = pl.ds(_aligned(j * BLOCK, BLOCK), BLOCK)
            scores = [_dot(k_s[h, keys, :], q_s[h, rows, :], 1, 1) for h in range(heads)]
            weights, keeps = [], []
            if masked:
                ok = lax.broadcasted_iota(jnp.int32, (BLOCK, BLOCK), 1) >= lax.broadcasted_iota(jnp.int32, (BLOCK, BLOCK), 0)
            for h, s in enumerate(scores):
                if masked:
                    s = jnp.where(ok, s, HIDDEN)
                old = top_s[h : h + 1, :]
                top = jnp.maximum(old, s.max(axis=0, keepdims=True))
                top_s[h : h + 1, :] = top
                weights.append(jnp.exp2((s - top) * e).astype(jnp.bfloat16))
                keeps.append(jnp.exp2((old - top) * e))
            for h, (p, keep) in enumerate(zip(weights, keeps)):
                mix_s[h] = mix_s[h] * keep + _dot(vt_s[h, :, keys], p, 1, 0)

        last = lax.div(row, BLOCK)
        lax.fori_loop(0, last, lambda j, _: step(j, False), None)
        step(last, True)
        for h in range(heads):
            out = (mix_s[h, :HEAD, :] * (1 / mix_s[h, HEAD : HEAD + 1, :])).astype(seen_s.dtype)
            seen_s[c, rows, h * HEAD : (h + 1) * HEAD] = out.T

    def seen_out(s):
        rows = pl.ds(_aligned(there + s * BLOCK + (1 - c) * HALF, HALF), HALF)
        return remote(seen_s.at[c, rows, :], seen_s.at[c, rows, :], seen_send, seen_recv, mate)

    def seen_in(s):
        rows = pl.ds(_aligned(there + s * BLOCK + c * HALF, HALF), HALF)
        return remote(seen_s.at[1 - c, rows, :], seen_s.at[1 - c, rows, :], seen_send, seen_recv, mate)

    def term_out(block, at, rows, to, i):
        src = term_s.at[pl.ds(block * HALF + at, rows), :]
        dst = got_s.at[pl.ds(_aligned((2 * c + block % 2) * HALF + at, 16), rows), :]
        return remote(src, dst, row_send, term_recv.at[i], 2 * (1 - chip) + to)

    def term(s):
        seen_in(s).wait_recv()
        rows = pl.ds(_aligned(there + s * BLOCK + c * HALF, HALF), HALF)
        a, b = seen_s[0, rows, :], seen_s[1, rows, :]
        for n in range(0, width, 512):
            t = _dot(a, wo_s[0, :, n : n + 512], 1, 0) + _dot(b, wo_s[1, :, n : n + 512], 1, 0)
            term_s[pl.ds(_aligned(s * HALF, HALF), HALF), n : n + 512] = t.astype(term_s.dtype)

    vt_s[:, HEAD:, :] = jnp.ones((heads, PAD, 4 * own), vt_s.dtype)
    load_turn.wait()
    pltpu.make_async_copy(w_s, w_s, load_sem.at[1]).wait()
    project(mine)

    @on_core(0)
    def _():
        near_in.wait_recv()
        far(2, here).start()
        far(3, here).start()


    def local(i, _):
        at = lax.rem(2 * c + 1 + i, 4)
        project(here + at * BLOCK)
        return _

    lax.fori_loop(0, 3, local, None)
    share_wo_in.wait_recv()
    share_wo.wait_send()

    def arrived(s, _):
        far(s, there).wait_recv()

        @pl.when(s == 2 * c)
        def _():
            at = there + c * own + first
            norm(LEAD, xn_s, at, at)

        @pl.when(s > 0)
        def _():
            term(s - 1)

        @pl.when(s == 2)
        def _():
            term_out(0, 0, 2 * HALF, 0, 0).start()

        @pl.when(s == 3)
        def _():
            term_out(2, 0, HALF, 1, 0).start()

        onward(s).start()
        onward_in(s).wait_recv()
        project(there + s * BLOCK)
        attend(there + s * BLOCK)
        seen_out(s).start()
        return _

    lax.fori_loop(0, 4, arrived, None)

    def mine_out(i):
        rows = pl.ds(_aligned(mates + i * BLOCK, BLOCK), BLOCK)
        return remote(seen_s.at[c, rows, :], seen_s.at[c, rows, :], seen_send, near_recv, mate)

    own_rows = pl.ds(_aligned(mine, BLOCK), own)
    mine_in = remote(seen_s.at[1 - c, own_rows, :], seen_s.at[1 - c, own_rows, :], seen_send, near_recv, mate)

    def inside(i, _):
        at = lax.rem(2 * (1 - c) + i, 4)
        attend(here + at * BLOCK)

        @pl.when(i == 0)
        def _():
            term(3)
            for i, (first_row, rows) in enumerate(LAST):
                term_out(3, first_row, rows, 1, 1 + i).start()

        @pl.when(i < 2)
        def _():
            mine_out(i).start()

        return _

    lax.fori_loop(0, 4, inside, None)

    def keep(i, _):
        rows = pl.ds(_aligned(mine + i * BLOCK, BLOCK), BLOCK)
        to = pl.ds(_aligned(i * BLOCK, BLOCK), BLOCK)
        a, b = seen_s[0, rows, :], seen_s[1, rows, :]
        for n in range(0, width, 512):
            t = _dot(a, wo_s[0, :, n : n + 512], 1, 0) + _dot(b, wo_s[1, :, n : n + 512], 1, 0)
            acc_s[to, n : n + 512] = t + x_s[to, n : n + 512].astype(jnp.float32)
        return _

    mine_in.wait_recv()
    lax.fori_loop(0, 2, keep, None)

    def terms_in(rows, i):
        rows = pl.ds(0, 2 * rows)
        remote(got_s.at[rows, :], got_s.at[rows, :], row_send, term_recv.at[i], peer).wait_recv()

    def finish(block, first, rows):
        for j in range(2):

            def some(r, _):
                at = pl.ds(_aligned((2 * block + j) * HALF + first + r * 16, 16), 16)
                got = pl.ds(_aligned((2 * j + block) * HALF + first + r * 16, 16), 16)
                y_ref[at, :] = (acc_s[at, :] + got_s[got, :].astype(jnp.float32)).astype(y_ref.dtype)
                return _

            lax.fori_loop(0, rows // 16, some, None)

    @on_core(0)
    def _():
        terms_in(2 * HALF, 0)
        finish(0, 0, HALF)
        finish(1, 0, HALF)

    @on_core(1)
    def _():
        terms_in(HALF, 0)
        finish(0, 0, HALF)
        for i, (first_row, rows) in enumerate(LAST):
            terms_in(rows, 1 + i)
            finish(1, first_row, rows)

    remote(xn_s, xn_s, row_send, near_recv, mate).wait_send()
    half_seen = seen_s.at[0, pl.ds(0, 2 * own), :]
    remote(half_seen, half_seen, seen_send, near_recv, mate).wait_send()


def _tables(tokens):
    half = HEAD // 2
    rate = np.float32(THETA) ** (-np.arange(half, dtype=np.float32) / np.float32(half))
    sign = np.concatenate([-np.ones(half), np.ones(half)])

    def pair(place):
        angle = place[:, None].astype(np.float64) * np.tile(rate, 2).astype(np.float64)
        return np.cos(angle).astype(np.float32), (np.sin(angle) * sign).astype(np.float32)

    both = zip(pair(np.arange(BLOCK)), pair(np.arange(0, tokens, BLOCK)))
    return np.stack([np.concatenate(t) for t in both])


def solution(mesh):
    def step(x, gain, wq, wk, wv, wo):
        own, width = x.shape
        tokens = 4 * own
        inner = wq.shape[1]
        heads = inner // HEAD
        low = jnp.bfloat16
        dma = pltpu.SemaphoreType.DMA
        hbm = pl.BlockSpec(memory_space=pl.ANY)
        return pl.pallas_call(
            functools.partial(kernel, own),
            name="layer",
            out_shape=pltpu.VMEM((own, width), low),
            in_specs=[hbm] * 7,
            out_specs=pl.BlockSpec(memory_space=pltpu.VMEM),
            scratch_shapes=[
                pltpu.VMEM((own, width), low),
                pltpu.VMEM((width // 128, 128), low),
                pltpu.VMEM((2, BLOCK + tokens // BLOCK, HEAD), jnp.float32),
                pltpu.VMEM((tokens, width), low),
                pltpu.VMEM((3, width, inner), low),
                pltpu.VMEM((2, inner, width), low),
                pltpu.VMEM((heads, tokens, HEAD), low),
                pltpu.VMEM((heads, tokens, HEAD), low),
                pltpu.VMEM((heads, HEAD + PAD, tokens), low),
                pltpu.VMEM((2, tokens, inner), low),
                pltpu.VMEM((8, BLOCK), jnp.float32),
                pltpu.VMEM((heads, HEAD + PAD, BLOCK), jnp.float32),
                pltpu.VMEM((own, width), low),
                pltpu.VMEM((own, width), low),
                pltpu.VMEM((own, width), jnp.float32),
                dma((2,)), pltpu.SemaphoreType.REGULAR, dma, dma,
                dma, dma((4,)), dma, dma, dma, dma((3,)),
            ],
            compiler_params=pltpu.CompilerParams(collective_id=0, has_side_effects=True, vmem_limit_bytes=VMEM),
        )(x, gain.reshape(width // 128, 128), wq, wk, wv, wo, jnp.asarray(_tables(tokens)))

    tokens, columns = P(("dp", "tp"), None), P(None, "tp")
    return jax.shard_map(
        step,
        mesh=mesh,
        in_specs=(tokens, P(None), columns, columns, columns, P("tp", None)),
        out_specs=tokens,
        check_vma=False,
    )
```

```python
import functools

import jax
import jax.numpy as jnp
import numpy as np
from jax import lax
from jax.experimental import pallas as pl
from jax.experimental.pallas import tpu as pltpu
from jax.sharding import PartitionSpec as P

HEAD = 128
THETA = 10000
VMEM = 60 * 2**20
NEG = float(np.finfo(np.float32).min)
HIDDEN = -np.inf
LOG2E = 1.4426950408889634
MESH = pl.DeviceIdType.MESH
BLOCK = 256
HALF = BLOCK // 2
LEAD = 32
LAST = (0, 112), (112, 16)
PAD = 16


def _dot(a, b, ca, cb):
    return lax.dot_general(a, b, (((ca,), (cb,)), ((), ())), preferred_element_type=jnp.float32)


def _aligned(x, n):
    return pl.multiple_of(x, n)


def kernel(own, x_hbm, gain_hbm, wq_hbm, wk_hbm, wv_hbm, wo_hbm, turn_hbm, y_ref,
           x_s, gain_s, turn_s, xn_s, w_s, wo_s, q_s, k_s, vt_s, seen_s, top_s, mix_s, term_s, got_s, acc_s,
           load_sem, mate_sem, row_send, seen_send, near_recv, far_recv, pass_recv, seen_recv, wo_recv, term_recv):
    heads = q_s.shape[0]
    width = x_s.shape[1]
    inner = heads * HEAD
    tp = lax.axis_index("tp")
    c = lax.rem(tp, 2)
    chip = lax.div(tp, 2)
    mate = tp + 1 - 2 * c
    peer = lax.rem(tp + 2, 4)
    here = chip * (2 * own)
    there = (1 - chip) * (2 * own)
    mine = here + c * own
    mates = here + (1 - c) * own

    def remote(src, dst, send, recv, device):
        return pltpu.make_async_remote_copy(src_ref=src, dst_ref=dst, send_sem=send, recv_sem=recv, device_id={"tp": device}, device_id_type=MESH)

    first = c * HALF
    order = [lax.rem(c + i, 4) for i in range(4)]

    def load_x(i, at, rows):
        rows = pl.ds(_aligned(at, LEAD), rows)
        return pltpu.make_async_copy(x_hbm.at[rows, :], x_s.at[rows, :], load_sem.at[i])

    loads_x = [load_x(1, order[0] * HALF, HALF), *(load_x(2, order[i] * HALF, HALF) for i in range(1, 4))]

    def load_w(i):
        return pltpu.make_async_copy((wq_hbm, wk_hbm, wv_hbm)[i], w_s.at[i], load_sem.at[1])

    load_wo = pltpu.make_async_copy(wo_hbm, wo_s.at[c], load_sem.at[2])
    load_gain = pltpu.make_async_copy(gain_hbm, gain_s, load_sem.at[0])
    load_turn = pltpu.make_async_copy(turn_hbm, turn_s, load_sem.at[0])

    def on_core(n):
        return pl.when(c == n)

    barrier = pltpu.get_barrier_semaphore()
    pl.semaphore_signal(barrier, inc=1, device_id={"tp": peer}, device_id_type=MESH)

    @on_core(1)
    def _():
        pl.semaphore_signal(barrier, inc=1, device_id={"tp": mate}, device_id_type=MESH)

    def near_rows(base, i, rows):
        rows = pl.ds(_aligned(base + i * HALF, HALF), rows)
        return remote(xn_s.at[rows, :], xn_s.at[rows, :], row_send, near_recv, mate)

    def near(i):
        return near_rows(mine, i, HALF)

    near_in = near_rows(mates, 0, own)

    def cross(base, at, rows, i):
        rows = pl.ds(_aligned(base + c * HALF + at, LEAD), rows)
        return remote(xn_s.at[rows, :], xn_s.at[rows, :], row_send, far_recv.at[i], peer)

    def far(s, base):
        return cross(base, s * BLOCK, HALF, s)

    def rest(base):
        return cross(base, 2 * c * BLOCK + LEAD, HALF - LEAD, 2 * c)

    def lead():
        to = pl.ds(_aligned(mine + first, LEAD), LEAD)
        return remote(x_hbm.at[pl.ds(_aligned(first, LEAD), LEAD), :], xn_s.at[to, :], row_send, far_recv.at[2 * c], peer)

    def onward(s):
        rows = pl.ds(_aligned(there + s * BLOCK + c * HALF, HALF), HALF)
        return remote(xn_s.at[rows, :], xn_s.at[rows, :], row_send, pass_recv, mate)

    def onward_in(s):
        rows = pl.ds(_aligned(there + s * BLOCK + (1 - c) * HALF, HALF), HALF)
        return remote(xn_s.at[rows, :], xn_s.at[rows, :], row_send, pass_recv, mate)

    def norm(rows, ref, at, to):
        def some(r, _):
            wide = ref[pl.ds(_aligned(at + r * 32, 32), 32), :].astype(jnp.float32)
            scale = lax.rsqrt(jnp.mean(wide * wide, -1, keepdims=True) + 1e-6)
            for g in range(width // 128):
                lanes = slice(g * 128, (g + 1) * 128)
                normed = wide[:, lanes] * scale * gain_s[g : g + 1, :].astype(jnp.float32)
                xn_s[pl.ds(_aligned(to + r * 32, 32), 32), lanes] = normed.astype(xn_s.dtype)
            return _

        lax.fori_loop(0, rows // 32, some, None)

    def tell_mate():
        pl.semaphore_signal(mate_sem, inc=1, device_id={"tp": mate}, device_id_type=MESH)

    @on_core(0)
    def _():
        pl.semaphore_wait(barrier, 2)
        tell_mate()

    @on_core(1)
    def _():
        pl.semaphore_wait(barrier, 1)

    lead().start()
    load_gain.start()
    for load in loads_x:
        load.start()
    load_gain.wait()
    load_turn.start()
    load_x(1, 0, HALF).wait()
    for i in range(3):
        load_w(i).start()
    norm(HALF, x_s, first, mine + first)

    @on_core(0)
    def _():
        rest(here).start()

    @on_core(1)
    def _():
        pl.semaphore_wait(mate_sem, 1)
        tell_mate()

    near(order[0]).start()
    load_x(2, 0, 3 * HALF).wait()
    load_wo.start()
    for i in range(1, 4):
        norm(HALF, x_s, order[i] * HALF, mine + order[i] * HALF)
        near(order[i]).start()
        if i == 2:

            @on_core(0)
            def _():
                far(1, here).start()

    @on_core(0)
    def _():
        pl.semaphore_wait(mate_sem, 1)

    @on_core(1)
    def _():
        near_in.wait_recv()
        far(0, here).start()
        far(1, here).start()
        rest(here).start()
        far(3, here).start()

    load_wo.wait()
    share_wo = remote(wo_s.at[c], wo_s.at[c], seen_send, wo_recv, mate)
    share_wo_in = remote(wo_s.at[1 - c], wo_s.at[1 - c], seen_send, wo_recv, mate)
    share_wo.start()

    def project(row):
        row = _aligned(row, BLOCK)
        rows = pl.ds(row, BLOCK)
        a = xn_s[rows, :]
        block = lax.div(row, BLOCK)
        cos_in, sin_in = turn_s[0, :BLOCK, :], turn_s[1, :BLOCK, :]
        cb, sb = turn_s[0, pl.ds(BLOCK + block, 1), :], turn_s[1, pl.ds(BLOCK + block, 1), :]
        cos = cb * cos_in - sb * sin_in
        sin = sb * cos_in + cb * sin_in
        for i, to in ((0, q_s), (1, k_s)):
            t = _dot(a, w_s[i], 1, 0).astype(jnp.bfloat16)
            for h in range(heads):
                u = t[:, h * HEAD : (h + 1) * HEAD].astype(jnp.float32)
                to[h, rows, :] = (u * cos + pltpu.roll(u, HEAD // 2, 1) * sin).astype(to.dtype)
        t = _dot(a, w_s[2], 1, 0).astype(jnp.bfloat16)
        for h in range(heads):
            vt_s[h, :HEAD, rows] = t[:, h * HEAD : (h + 1) * HEAD].T

    e = HEAD**-0.5 * LOG2E

    def attend(row):
        row = _aligned(row, BLOCK)
        rows = pl.ds(row, BLOCK)
        top_s[...] = jnp.full(top_s.shape, NEG, jnp.float32)
        mix_s[...] = jnp.zeros(mix_s.shape, jnp.float32)

        def step(j, masked):
            keys = pl.ds(_aligned(j * BLOCK, BLOCK), BLOCK)
            scores = [_dot(k_s[h, keys, :], q_s[h, rows, :], 1, 1) for h in range(heads)]
            weights, keeps = [], []
            if masked:
                ok = lax.broadcasted_iota(jnp.int32, (BLOCK, BLOCK), 1) >= lax.broadcasted_iota(jnp.int32, (BLOCK, BLOCK), 0)
            for h, s in enumerate(scores):
                if masked:
                    s = jnp.where(ok, s, HIDDEN)
                old = top_s[h : h + 1, :]
                top = jnp.maximum(old, s.max(axis=0, keepdims=True))
                top_s[h : h + 1, :] = top
                weights.append(jnp.exp2((s - top) * e).astype(jnp.bfloat16))
                keeps.append(jnp.exp2((old - top) * e))
            for h, (p, keep) in enumerate(zip(weights, keeps)):
                mix_s[h] = mix_s[h] * keep + _dot(vt_s[h, :, keys], p, 1, 0)

        last = lax.div(row, BLOCK)
        lax.fori_loop(0, last, lambda j, _: step(j, False), None)
        step(last, True)
        for h in range(heads):
            out = (mix_s[h, :HEAD, :] * (1 / mix_s[h, HEAD : HEAD + 1, :])).astype(seen_s.dtype)
            seen_s[c, rows, h * HEAD : (h + 1) * HEAD] = out.T

    def seen_out(s):
        rows = pl.ds(_aligned(there + s * BLOCK + (1 - c) * HALF, HALF), HALF)
        return remote(seen_s.at[c, rows, :], seen_s.at[c, rows, :], seen_send, seen_recv, mate)

    def seen_in(s):
        rows = pl.ds(_aligned(there + s * BLOCK + c * HALF, HALF), HALF)
        return remote(seen_s.at[1 - c, rows, :], seen_s.at[1 - c, rows, :], seen_send, seen_recv, mate)

    def term_out(block, at, rows, to, i):
        src = term_s.at[pl.ds(block * HALF + at, rows), :]
        dst = got_s.at[pl.ds(_aligned((2 * c + block % 2) * HALF + at, 16), rows), :]
        return remote(src, dst, row_send, term_recv.at[i], 2 * (1 - chip) + to)

    def term(s):
        seen_in(s).wait_recv()
        rows = pl.ds(_aligned(there + s * BLOCK + c * HALF, HALF), HALF)
        a, b = seen_s[0, rows, :], seen_s[1, rows, :]
        for n in range(0, width, 512):
            t = _dot(a, wo_s[0, :, n : n + 512], 1, 0) + _dot(b, wo_s[1, :, n : n + 512], 1, 0)
            term_s[pl.ds(_aligned(s * HALF, HALF), HALF), n : n + 512] = t.astype(term_s.dtype)

    vt_s[:, HEAD:, :] = jnp.ones((heads, PAD, 4 * own), vt_s.dtype)
    load_turn.wait()
    pltpu.make_async_copy(w_s, w_s, load_sem.at[1]).wait()
    project(mine)

    @on_core(0)
    def _():
        near_in.wait_recv()
        far(2, here).start()
        far(3, here).start()


    def local(i, _):
        at = lax.rem(2 * c + 1 + i, 4)
        project(here + at * BLOCK)
        return _

    lax.fori_loop(0, 3, local, None)
    share_wo_in.wait_recv()
    share_wo.wait_send()

    def arrived(s, _):
        far(s, there).wait_recv()

        @pl.when(s == 2 * c)
        def _():
            at = there + c * own + first
            norm(LEAD, xn_s, at, at)

        @pl.when(s > 0)
        def _():
            term(s - 1)

        @pl.when(s == 2)
        def _():
            term_out(0, 0, 2 * HALF, 0, 0).start()

        @pl.when(s == 3)
        def _():
            term_out(2, 0, HALF, 1, 0).start()

        onward(s).start()
        onward_in(s).wait_recv()
        project(there + s * BLOCK)
        attend(there + s * BLOCK)
        seen_out(s).start()
        return _

    lax.fori_loop(0, 4, arrived, None)

    def mine_out(i):
        rows = pl.ds(_aligned(mates + i * BLOCK, BLOCK), BLOCK)
        return remote(seen_s.at[c, rows, :], seen_s.at[c, rows, :], seen_send, near_recv, mate)

    own_rows = pl.ds(_aligned(mine, BLOCK), own)
    mine_in = remote(seen_s.at[1 - c, own_rows, :], seen_s.at[1 - c, own_rows, :], seen_send, near_recv, mate)

    def inside(i, _):
        at = lax.rem(2 * (1 - c) + i, 4)
        attend(here + at * BLOCK)

        @pl.when(i == 0)
        def _():
            term(3)
            for i, (first_row, rows) in enumerate(LAST):
                term_out(3, first_row, rows, 1, 1 + i).start()

        @pl.when(i < 2)
        def _():
            mine_out(i).start()

        return _

    lax.fori_loop(0, 4, inside, None)

    def keep(i, _):
        rows = pl.ds(_aligned(mine + i * BLOCK, BLOCK), BLOCK)
        to = pl.ds(_aligned(i * BLOCK, BLOCK), BLOCK)
        a, b = seen_s[0, rows, :], seen_s[1, rows, :]
        for n in range(0, width, 512):
            t = _dot(a, wo_s[0, :, n : n + 512], 1, 0) + _dot(b, wo_s[1, :, n : n + 512], 1, 0)
            acc_s[to, n : n + 512] = t + x_s[to, n : n + 512].astype(jnp.float32)
        return _

    mine_in.wait_recv()
    lax.fori_loop(0, 2, keep, None)

    def terms_in(rows, i):
        rows = pl.ds(0, 2 * rows)
        remote(got_s.at[rows, :], got_s.at[rows, :], row_send, term_recv.at[i], peer).wait_recv()

    def finish(block, first, rows):
        for j in range(2):

            def some(r, _):
                at = pl.ds(_aligned((2 * block + j) * HALF + first + r * 16, 16), 16)
                got = pl.ds(_aligned((2 * j + block) * HALF + first + r * 16, 16), 16)
                y_ref[at, :] = (acc_s[at, :] + got_s[got, :].astype(jnp.float32)).astype(y_ref.dtype)
                return _

            lax.fori_loop(0, rows // 16, some, None)

    @on_core(0)
    def _():
        terms_in(2 * HALF, 0)
        finish(0, 0, HALF)
        finish(1, 0, HALF)

    @on_core(1)
    def _():
        terms_in(HALF, 0)
        finish(0, 0, HALF)
        for i, (first_row, rows) in enumerate(LAST):
            terms_in(rows, 1 + i)
            finish(1, first_row, rows)

    remote(xn_s, xn_s, row_send, near_recv, mate).wait_send()
    half_seen = seen_s.at[0, pl.ds(0, 2 * own), :]
    remote(half_seen, half_seen, seen_send, near_recv, mate).wait_send()


def _tables(tokens):
    half = HEAD // 2
    rate = np.float32(THETA) ** (-np.arange(half, dtype=np.float32) / np.float32(half))
    sign = np.concatenate([-np.ones(half), np.ones(half)])

    def pair(place):
        angle = place[:, None].astype(np.float64) * np.tile(rate, 2).astype(np.float64)
        return np.cos(angle).astype(np.float32), (np.sin(angle) * sign).astype(np.float32)

    both = zip(pair(np.arange(BLOCK)), pair(np.arange(0, tokens, BLOCK)))
    return np.stack([np.concatenate(t) for t in both])


def solution(mesh):
    def step(x, gain, wq, wk, wv, wo):
        own, width = x.shape
        tokens = 4 * own
        inner = wq.shape[1]
        heads = inner // HEAD
        low = jnp.bfloat16
        dma = pltpu.SemaphoreType.DMA
        hbm = pl.BlockSpec(memory_space=pl.ANY)
        return pl.pallas_call(
            functools.partial(kernel, own),
            name="layer",
            out_shape=pltpu.VMEM((own, width), low),
            in_specs=[hbm] * 7,
            out_specs=pl.BlockSpec(memory_space=pltpu.VMEM),
            scratch_shapes=[
                pltpu.VMEM((own, width), low),
                pltpu.VMEM((width // 128, 128), low),
                pltpu.VMEM((2, BLOCK + tokens // BLOCK, HEAD), jnp.float32),
                pltpu.VMEM((tokens, width), low),
                pltpu.VMEM((3, width, inner), low),
                pltpu.VMEM((2, inner, width), low),
                pltpu.VMEM((heads, tokens, HEAD), low),
                pltpu.VMEM((heads, tokens, HEAD), low),
                pltpu.VMEM((heads, HEAD + PAD, tokens), low),
                pltpu.VMEM((2, tokens, inner), low),
                pltpu.VMEM((8, BLOCK), jnp.float32),
                pltpu.VMEM((heads, HEAD + PAD, BLOCK), jnp.float32),
                pltpu.VMEM((own, width), low),
                pltpu.VMEM((own, width), low),
                pltpu.VMEM((own, width), jnp.float32),
                dma((3,)), pltpu.SemaphoreType.REGULAR, dma, dma,
                dma, dma((4,)), dma, dma, dma, dma((3,)),
            ],
            compiler_params=pltpu.CompilerParams(collective_id=0, has_side_effects=True, vmem_limit_bytes=VMEM),
        )(x, gain.reshape(width // 128, 128), wq, wk, wv, wo, jnp.asarray(_tables(tokens)))

    tokens, columns = P(("dp", "tp"), None), P(None, "tp")
    return jax.shard_map(
        step,
        mesh=mesh,
        in_specs=(tokens, P(None), columns, columns, columns, P("tp", None)),
        out_specs=tokens,
        check_vma=False,
    )
```

```python
import functools

import jax
import jax.numpy as jnp
import numpy as np
from jax import lax
from jax.experimental import pallas as pl
from jax.experimental.pallas import tpu as pltpu
from jax.sharding import PartitionSpec as P

HEAD = 128
THETA = 10000
VMEM = 60 * 2**20
NEG = float(np.finfo(np.float32).min)
HIDDEN = -np.inf
LOG2E = 1.4426950408889634
MESH = pl.DeviceIdType.MESH
BLOCK = 256
HALF = BLOCK // 2
LEAD = 32
LAST = (0, 112), (112, 16)
PAD = 16


def _dot(a, b, ca, cb):
    return lax.dot_general(a, b, (((ca,), (cb,)), ((), ())), preferred_element_type=jnp.float32)


def _aligned(x, n):
    return pl.multiple_of(x, n)


def kernel(own, x_hbm, gain_hbm, wq_hbm, wk_hbm, wv_hbm, wo_hbm, turn_hbm, y_ref,
           x_s, gain_s, turn_s, xn_s, w_s, wo_s, q_s, k_s, vt_s, seen_s, top_s, mix_s, term_s, got_s, acc_s,
           load_sem, mate_sem, row_send, seen_send, near_recv, far_recv, pass_recv, seen_recv, wo_recv, term_recv):
    heads = q_s.shape[0]
    width = x_s.shape[1]
    inner = heads * HEAD
    tp = lax.axis_index("tp")
    c = lax.rem(tp, 2)
    chip = lax.div(tp, 2)
    mate = tp + 1 - 2 * c
    peer = lax.rem(tp + 2, 4)
    here = chip * (2 * own)
    there = (1 - chip) * (2 * own)
    mine = here + c * own
    mates = here + (1 - c) * own

    def remote(src, dst, send, recv, device):
        return pltpu.make_async_remote_copy(src_ref=src, dst_ref=dst, send_sem=send, recv_sem=recv, device_id={"tp": device}, device_id_type=MESH)

    first = c * HALF
    order = [lax.rem(c + i, 4) for i in range(4)]

    def load_x(i, at, rows):
        rows = pl.ds(_aligned(at, LEAD), rows)
        return pltpu.make_async_copy(x_hbm.at[rows, :], x_s.at[rows, :], load_sem.at[i])

    loads_x = [load_x(1, order[0] * HALF, HALF), *(load_x(2, order[i] * HALF, HALF) for i in range(1, 4))]

    def load_w(i):
        return pltpu.make_async_copy((wq_hbm, wk_hbm, wv_hbm)[i], w_s.at[i], load_sem.at[1])

    load_wo = pltpu.make_async_copy(wo_hbm, wo_s.at[c], load_sem.at[2])
    load_gain = pltpu.make_async_copy(gain_hbm, gain_s, load_sem.at[0])
    load_turn = pltpu.make_async_copy(turn_hbm, turn_s, load_sem.at[0])

    def on_core(n):
        return pl.when(c == n)

    barrier = pltpu.get_barrier_semaphore()
    pl.semaphore_signal(barrier, inc=1, device_id={"tp": peer}, device_id_type=MESH)

    @on_core(1)
    def _():
        pl.semaphore_signal(barrier, inc=1, device_id={"tp": mate}, device_id_type=MESH)

    def near_rows(base, i, rows):
        rows = pl.ds(_aligned(base + i * HALF, HALF), rows)
        return remote(xn_s.at[rows, :], xn_s.at[rows, :], row_send, near_recv, mate)

    def near(i):
        return near_rows(mine, i, HALF)

    near_in = near_rows(mates, 0, own)

    def cross(base, at, rows, i):
        rows = pl.ds(_aligned(base + c * HALF + at, LEAD), rows)
        return remote(xn_s.at[rows, :], xn_s.at[rows, :], row_send, far_recv.at[i], peer)

    def far(s, base):
        return cross(base, s * BLOCK, HALF, s)

    def rest(base):
        return cross(base, 2 * c * BLOCK + LEAD, HALF - LEAD, 2 * c)

    def lead():
        to = pl.ds(_aligned(mine + first, LEAD), LEAD)
        return remote(x_hbm.at[pl.ds(_aligned(first, LEAD), LEAD), :], xn_s.at[to, :], row_send, far_recv.at[2 * c], peer)

    def onward(s):
        rows = pl.ds(_aligned(there + s * BLOCK + c * HALF, HALF), HALF)
        return remote(xn_s.at[rows, :], xn_s.at[rows, :], row_send, pass_recv, mate)

    def onward_in(s):
        rows = pl.ds(_aligned(there + s * BLOCK + (1 - c) * HALF, HALF), HALF)
        return remote(xn_s.at[rows, :], xn_s.at[rows, :], row_send, pass_recv, mate)

    def norm(rows, ref, at, to):
        def some(r, _):
            wide = ref[pl.ds(_aligned(at + r * 32, 32), 32), :].astype(jnp.float32)
            scale = lax.rsqrt(jnp.mean(wide * wide, -1, keepdims=True) + 1e-6)
            for g in range(width // 128):
                lanes = slice(g * 128, (g + 1) * 128)
                normed = wide[:, lanes] * scale * gain_s[g : g + 1, :].astype(jnp.float32)
                xn_s[pl.ds(_aligned(to + r * 32, 32), 32), lanes] = normed.astype(xn_s.dtype)
            return _

        lax.fori_loop(0, rows // 32, some, None)

    def tell_mate():
        pl.semaphore_signal(mate_sem, inc=1, device_id={"tp": mate}, device_id_type=MESH)

    load_gain.start()
    for load in loads_x:
        load.start()

    @on_core(0)
    def _():
        pl.semaphore_wait(barrier, 2)
        tell_mate()

    @on_core(1)
    def _():
        pl.semaphore_wait(barrier, 1)

    lead().start()
    load_gain.wait()
    load_turn.start()
    load_x(1, 0, HALF).wait()
    for i in range(3):
        load_w(i).start()
    norm(HALF, x_s, first, mine + first)

    @on_core(0)
    def _():
        rest(here).start()

    @on_core(1)
    def _():
        pl.semaphore_wait(mate_sem, 1)
        tell_mate()

    near(order[0]).start()
    load_x(2, 0, 3 * HALF).wait()
    load_wo.start()
    for i in range(1, 4):
        norm(HALF, x_s, order[i] * HALF, mine + order[i] * HALF)
        near(order[i]).start()
        if i == 2:

            @on_core(0)
            def _():
                far(1, here).start()

    @on_core(0)
    def _():
        pl.semaphore_wait(mate_sem, 1)

    @on_core(1)
    def _():
        near_in.wait_recv()
        far(0, here).start()
        far(1, here).start()
        rest(here).start()
        far(3, here).start()

    load_wo.wait()
    share_wo = remote(wo_s.at[c], wo_s.at[c], seen_send, wo_recv, mate)
    share_wo_in = remote(wo_s.at[1 - c], wo_s.at[1 - c], seen_send, wo_recv, mate)
    share_wo.start()

    def project(row):
        row = _aligned(row, BLOCK)
        rows = pl.ds(row, BLOCK)
        a = xn_s[rows, :]
        block = lax.div(row, BLOCK)
        cos_in, sin_in = turn_s[0, :BLOCK, :], turn_s[1, :BLOCK, :]
        cb, sb = turn_s[0, pl.ds(BLOCK + block, 1), :], turn_s[1, pl.ds(BLOCK + block, 1), :]
        cos = cb * cos_in - sb * sin_in
        sin = sb * cos_in + cb * sin_in
        for i, to in ((0, q_s), (1, k_s)):
            t = _dot(a, w_s[i], 1, 0).astype(jnp.bfloat16)
            for h in range(heads):
                u = t[:, h * HEAD : (h + 1) * HEAD].astype(jnp.float32)
                to[h, rows, :] = (u * cos + pltpu.roll(u, HEAD // 2, 1) * sin).astype(to.dtype)
        t = _dot(a, w_s[2], 1, 0).astype(jnp.bfloat16)
        for h in range(heads):
            vt_s[h, :HEAD, rows] = t[:, h * HEAD : (h + 1) * HEAD].T

    e = HEAD**-0.5 * LOG2E

    def attend(row):
        row = _aligned(row, BLOCK)
        rows = pl.ds(row, BLOCK)
        top_s[...] = jnp.full(top_s.shape, NEG, jnp.float32)
        mix_s[...] = jnp.zeros(mix_s.shape, jnp.float32)

        def step(j, masked):
            keys = pl.ds(_aligned(j * BLOCK, BLOCK), BLOCK)
            scores = [_dot(k_s[h, keys, :], q_s[h, rows, :], 1, 1) for h in range(heads)]
            weights, keeps = [], []
            if masked:
                ok = lax.broadcasted_iota(jnp.int32, (BLOCK, BLOCK), 1) >= lax.broadcasted_iota(jnp.int32, (BLOCK, BLOCK), 0)
            for h, s in enumerate(scores):
                if masked:
                    s = jnp.where(ok, s, HIDDEN)
                old = top_s[h : h + 1, :]
                top = jnp.maximum(old, s.max(axis=0, keepdims=True))
                top_s[h : h + 1, :] = top
                weights.append(jnp.exp2((s - top) * e).astype(jnp.bfloat16))
                keeps.append(jnp.exp2((old - top) * e))
            for h, (p, keep) in enumerate(zip(weights, keeps)):
                mix_s[h] = mix_s[h] * keep + _dot(vt_s[h, :, keys], p, 1, 0)

        last = lax.div(row, BLOCK)
        lax.fori_loop(0, last, lambda j, _: step(j, False), None)
        step(last, True)
        for h in range(heads):
            out = (mix_s[h, :HEAD, :] * (1 / mix_s[h, HEAD : HEAD + 1, :])).astype(seen_s.dtype)
            seen_s[c, rows, h * HEAD : (h + 1) * HEAD] = out.T

    def seen_out(s):
        rows = pl.ds(_aligned(there + s * BLOCK + (1 - c) * HALF, HALF), HALF)
        return remote(seen_s.at[c, rows, :], seen_s.at[c, rows, :], seen_send, seen_recv, mate)

    def seen_in(s):
        rows = pl.ds(_aligned(there + s * BLOCK + c * HALF, HALF), HALF)
        return remote(seen_s.at[1 - c, rows, :], seen_s.at[1 - c, rows, :], seen_send, seen_recv, mate)

    def term_out(block, at, rows, to, i):
        src = term_s.at[pl.ds(block * HALF + at, rows), :]
        dst = got_s.at[pl.ds(_aligned((2 * c + block % 2) * HALF + at, 16), rows), :]
        return remote(src, dst, row_send, term_recv.at[i], 2 * (1 - chip) + to)

    def term(s):
        seen_in(s).wait_recv()
        rows = pl.ds(_aligned(there + s * BLOCK + c * HALF, HALF), HALF)
        a, b = seen_s[0, rows, :], seen_s[1, rows, :]
        for n in range(0, width, 512):
            t = _dot(a, wo_s[0, :, n : n + 512], 1, 0) + _dot(b, wo_s[1, :, n : n + 512], 1, 0)
            term_s[pl.ds(_aligned(s * HALF, HALF), HALF), n : n + 512] = t.astype(term_s.dtype)

    vt_s[:, HEAD:, :] = jnp.ones((heads, PAD, 4 * own), vt_s.dtype)
    load_turn.wait()
    pltpu.make_async_copy(w_s, w_s, load_sem.at[1]).wait()
    project(mine)

    @on_core(0)
    def _():
        near_in.wait_recv()
        far(2, here).start()
        far(3, here).start()


    def local(i, _):
        at = lax.rem(2 * c + 1 + i, 4)
        project(here + at * BLOCK)
        return _

    lax.fori_loop(0, 3, local, None)
    share_wo_in.wait_recv()
    share_wo.wait_send()

    def arrived(s, _):
        far(s, there).wait_recv()

        @pl.when(s == 2 * c)
        def _():
            at = there + c * own + first
            norm(LEAD, xn_s, at, at)

        @pl.when(s > 0)
        def _():
            term(s - 1)

        @pl.when(s == 2)
        def _():
            term_out(0, 0, 2 * HALF, 0, 0).start()

        @pl.when(s == 3)
        def _():
            term_out(2, 0, HALF, 1, 0).start()

        onward(s).start()
        onward_in(s).wait_recv()
        project(there + s * BLOCK)
        attend(there + s * BLOCK)
        seen_out(s).start()
        return _

    lax.fori_loop(0, 4, arrived, None)

    def mine_out(i):
        rows = pl.ds(_aligned(mates + i * BLOCK, BLOCK), BLOCK)
        return remote(seen_s.at[c, rows, :], seen_s.at[c, rows, :], seen_send, near_recv, mate)

    own_rows = pl.ds(_aligned(mine, BLOCK), own)
    mine_in = remote(seen_s.at[1 - c, own_rows, :], seen_s.at[1 - c, own_rows, :], seen_send, near_recv, mate)

    def inside(i, _):
        at = lax.rem(2 * (1 - c) + i, 4)
        attend(here + at * BLOCK)

        @pl.when(i == 0)
        def _():
            term(3)
            for i, (first_row, rows) in enumerate(LAST):
                term_out(3, first_row, rows, 1, 1 + i).start()

        @pl.when(i < 2)
        def _():
            mine_out(i).start()

        return _

    lax.fori_loop(0, 4, inside, None)

    def keep(i, _):
        rows = pl.ds(_aligned(mine + i * BLOCK, BLOCK), BLOCK)
        to = pl.ds(_aligned(i * BLOCK, BLOCK), BLOCK)
        a, b = seen_s[0, rows, :], seen_s[1, rows, :]
        for n in range(0, width, 512):
            t = _dot(a, wo_s[0, :, n : n + 512], 1, 0) + _dot(b, wo_s[1, :, n : n + 512], 1, 0)
            acc_s[to, n : n + 512] = t + x_s[to, n : n + 512].astype(jnp.float32)
        return _

    mine_in.wait_recv()
    lax.fori_loop(0, 2, keep, None)

    def terms_in(rows, i):
        rows = pl.ds(0, 2 * rows)
        remote(got_s.at[rows, :], got_s.at[rows, :], row_send, term_recv.at[i], peer).wait_recv()

    def finish(block, first, rows):
        for j in range(2):

            def some(r, _):
                at = pl.ds(_aligned((2 * block + j) * HALF + first + r * 16, 16), 16)
                got = pl.ds(_aligned((2 * j + block) * HALF + first + r * 16, 16), 16)
                y_ref[at, :] = (acc_s[at, :] + got_s[got, :].astype(jnp.float32)).astype(y_ref.dtype)
                return _

            lax.fori_loop(0, rows // 16, some, None)

    @on_core(0)
    def _():
        terms_in(2 * HALF, 0)
        finish(0, 0, HALF)
        finish(1, 0, HALF)

    @on_core(1)
    def _():
        terms_in(HALF, 0)
        finish(0, 0, HALF)
        for i, (first_row, rows) in enumerate(LAST):
            terms_in(rows, 1 + i)
            finish(1, first_row, rows)

    remote(xn_s, xn_s, row_send, near_recv, mate).wait_send()
    half_seen = seen_s.at[0, pl.ds(0, 2 * own), :]
    remote(half_seen, half_seen, seen_send, near_recv, mate).wait_send()


def _tables(tokens):
    half = HEAD // 2
    rate = np.float32(THETA) ** (-np.arange(half, dtype=np.float32) / np.float32(half))
    sign = np.concatenate([-np.ones(half), np.ones(half)])

    def pair(place):
        angle = place[:, None].astype(np.float64) * np.tile(rate, 2).astype(np.float64)
        return np.cos(angle).astype(np.float32), (np.sin(angle) * sign).astype(np.float32)

    both = zip(pair(np.arange(BLOCK)), pair(np.arange(0, tokens, BLOCK)))
    return np.stack([np.concatenate(t) for t in both])


def solution(mesh):
    def step(x, gain, wq, wk, wv, wo):
        own, width = x.shape
        tokens = 4 * own
        inner = wq.shape[1]
        heads = inner // HEAD
        low = jnp.bfloat16
        dma = pltpu.SemaphoreType.DMA
        hbm = pl.BlockSpec(memory_space=pl.ANY)
        return pl.pallas_call(
            functools.partial(kernel, own),
            name="layer",
            out_shape=pltpu.VMEM((own, width), low),
            in_specs=[hbm] * 7,
            out_specs=pl.BlockSpec(memory_space=pltpu.VMEM),
            scratch_shapes=[
                pltpu.VMEM((own, width), low),
                pltpu.VMEM((width // 128, 128), low),
                pltpu.VMEM((2, BLOCK + tokens // BLOCK, HEAD), jnp.float32),
                pltpu.VMEM((tokens, width), low),
                pltpu.VMEM((3, width, inner), low),
                pltpu.VMEM((2, inner, width), low),
                pltpu.VMEM((heads, tokens, HEAD), low),
                pltpu.VMEM((heads, tokens, HEAD), low),
                pltpu.VMEM((heads, HEAD + PAD, tokens), low),
                pltpu.VMEM((2, tokens, inner), low),
                pltpu.VMEM((8, BLOCK), jnp.float32),
                pltpu.VMEM((heads, HEAD + PAD, BLOCK), jnp.float32),
                pltpu.VMEM((own, width), low),
                pltpu.VMEM((own, width), low),
                pltpu.VMEM((own, width), jnp.float32),
                dma((3,)), pltpu.SemaphoreType.REGULAR, dma, dma,
                dma, dma((4,)), dma, dma, dma, dma((3,)),
            ],
            compiler_params=pltpu.CompilerParams(collective_id=0, has_side_effects=True, vmem_limit_bytes=VMEM),
        )(x, gain.reshape(width // 128, 128), wq, wk, wv, wo, jnp.asarray(_tables(tokens)))

    tokens, columns = P(("dp", "tp"), None), P(None, "tp")
    return jax.shard_map(
        step,
        mesh=mesh,
        in_specs=(tokens, P(None), columns, columns, columns, P("tp", None)),
        out_specs=tokens,
        check_vma=False,
    )
```
